256 devices in a mesh: probe: 4 (over y), space: 64 (over x, z, core).
Axes of the slice: x: 4, y: 4, z: 8, core: 2. Of those that a mesh axis runs over, the one named last changes fastest.
Arguments:
- probe_signs: int32 [192, 512, 1024], P('probe', 'space'), may hold values from 0 to 1, as said below
- sensor_mask: int32 [512, 1024], P('space'), may hold values 0 or 1
- sensor_weight: float32 [512, 1024], P('space'), may hold values from 1 to 30
- prior_mass: float32 [512, 1024], P('space'), may hold values from 0.02 to 0.5
Outputs:
- solution: float32 [192, 512, 1024], P('probe', 'space')
- trace_cell: float32 [], replicated
The draws below stay inside these ranges and needn't reach their ends.
Inputs may be any that keep to these rules, and one draw needn't show every extreme that they name: `probe_signs`: each entry is 0 or 1; the probe's sign is twice the entry minus one.
All inputs are finite; a program needn't handle non-finite values. No bound on the sum of `sensor_mask` on one device may be relied on, other than what follows from the above.
Results may differ from the reference program's by a relative error of at most 0.0001.
Values sent between devices are 32-bit elements; how exact they have to be, the bound alone decides.
No kernel may reach another device: no remote copies, remote signals or barrier semaphores. Data moves between devices by JAX's collectives and lax.ppermute only.
A program may use at most 64 MiB of HBM per device.

```python
import math
import jax
import jax.numpy as jnp
from jax import lax

PROBES_DEV = 48
ITERS = 4
NX = 512
NY = 1024
PROBES = 192


def draw_probe_signs(key, part):
    levels = 1048576
    probe_index = jnp.arange(PROBES, dtype=jnp.int32)
    threshold = 524288 + 471859 * probe_index // max(PROBES - 1, 1)
    uniform_bits = jax.random.randint(jax.random.fold_in(key, 17), (PROBES, NX, NY), 0, levels, dtype=jnp.int32)
    return (uniform_bits < threshold[:, None, None]).astype(jnp.int32)


def place_ends(drawn, stream_key, low, high):
    spot = [jax.random.randint(jax.random.fold_in(stream_key, axis), (), 0, length) for axis, length in enumerate(drawn.shape)]
    widest = drawn.shape.index(max(drawn.shape))
    neighbour = spot[:widest] + [(spot[widest] + 1) % drawn.shape[widest]] + spot[widest + 1:]
    return drawn.at[tuple(spot)].set(low).at[tuple(neighbour)].set(high)


def shard_levels(stream_key, dims, pieces, low, top_value):
    level, own = 1.0, jax.random.fold_in(stream_key, 6)
    for axis_at, blocks in pieces:
        steps = jnp.exp(jax.random.uniform(jax.random.fold_in(own, axis_at), (blocks,), jnp.float32, low / len(pieces), top_value / len(pieces)))
        level = level * jnp.repeat(steps, dims[axis_at] // blocks).reshape([-1 if axis == axis_at else 1 for axis in range(len(dims))])
    return level


def setup_inputs(seed: int = 0) -> dict:
    arg_keys = jax.random.split(jax.random.key(seed), 5)
    probe_signs = draw_probe_signs(jax.random.fold_in(arg_keys[4], 71), 0)
    sensor_mask = place_ends((jax.random.randint(arg_keys[1], (NX, NY), 0, 8) < 1).astype(jnp.int32), jax.random.fold_in(arg_keys[1], 1), 0, 1)
    sensor_weight = jnp.clip(jnp.exp(math.log(30.0) - 3.4011974 * jax.random.uniform(arg_keys[2], (NX, NY), jnp.float32) ** shard_levels(arg_keys[2], (NX, NY), ((0, 64),), -0.2, 0.2)), 1.0, 30.0)
    prior_mass = jnp.clip(jnp.exp(math.log(0.5) - 3.218876 * jax.random.uniform(arg_keys[3], (NX, NY), jnp.float32) ** shard_levels(arg_keys[3], (NX, NY), ((0, 64),), -0.2, 0.2)), 0.02, 0.5)
    return {"probe_signs": probe_signs, "sensor_mask": sensor_mask, "sensor_weight": sensor_weight, "prior_mass": prior_mass}


def operate(vector_in, diagonal):
    padded = jnp.pad(vector_in, ((0, 0), (1, 1), (1, 1)))
    beside = padded[:, 2:, 1:-1] + padded[:, :-2, 1:-1]
    beside = beside + padded[:, 1:-1, 2:] + padded[:, 1:-1, :-2]
    return (4.0 + diagonal) * vector_in - beside


def solve_block(probe_block, diagonal):
    probes = 2.0 * probe_block.astype(jnp.float32) - 1.0
    solution = jnp.zeros_like(probes)
    residual = probes
    direction = probes
    norm_now = jnp.sum(residual * residual, axis=(1, 2))
    for iterate in range(ITERS):
        applied = operate(direction, diagonal)
        step_len = norm_now / jnp.sum(direction * applied, axis=(1, 2))
        solution = solution + step_len[:, None, None] * direction
        residual = residual - step_len[:, None, None] * applied
        norm_next = jnp.sum(residual * residual, axis=(1, 2))
        direction = residual + (norm_next / norm_now)[:, None, None] * direction
        norm_now = norm_next
    return solution, jnp.sum(probes * solution)


def reference(probe_signs, sensor_mask, sensor_weight, prior_mass):
    diagonal = sensor_mask.astype(jnp.float32) * sensor_weight + prior_mass
    blocks = probe_signs.reshape(PROBES // PROBES_DEV, PROBES_DEV, NX, NY)

    def one_block(probe_block):
        return solve_block(probe_block, diagonal)

    solutions, partial_sums = lax.map(one_block, blocks)
    solution = solutions.reshape(PROBES, NX, NY)
    trace_cell = jnp.sum(partial_sums) / float(PROBES * NX * NY)
    return solution, trace_cell
```

```python
import functools

import jax
import jax.numpy as jnp
from jax import lax
from jax.experimental import pallas as pl
from jax.experimental.pallas import tpu as pltpu
from jax.sharding import PartitionSpec as P

ITERS = 4
SHIFT = 6.0
LANES = 128
BLOCK = 8


def powers_kernel(
    signs_ref, dd_ref, up_ref, up_dd_ref, dn_ref, dn_dd_ref, mask_ref,
    v1_ref, v2_ref, v3_ref, sums_ref, halo_ref, dd_halo_ref, part_ref,
):
    step = pl.program_id(0)
    tiles = dd_ref.shape[1] // LANES
    sub = lax.broadcasted_iota(jnp.int32, (8, LANES), 0)
    lane = lax.broadcasted_iota(jnp.int32, (8, LANES), 1)
    top, bottom = sub == 0, sub == 7
    first, last = lane == 0, lane == LANES - 1
    nothing = jnp.zeros((8, LANES), jnp.float32)
    valid = mask_ref[...]

    @pl.when(step == 0)
    def _():
        halo_ref[...] = jnp.zeros_like(halo_ref)
        dd_halo_ref[...] = jnp.zeros_like(dd_halo_ref)
        dd_halo_ref[0:4, :] = up_dd_ref[0]
        dd_halo_ref[5:8, :] = dn_dd_ref[0]
        part_ref[...] = jnp.zeros_like(part_ref)

    def at(c):
        return pl.ds(c * LANES, LANES)

    def sideways(v):
        left = [pltpu.roll(t, 1, 1) for t in v]
        right = [pltpu.roll(t, LANES - 1, 1) for t in v]
        out = []
        for c in range(tiles):
            a = jnp.where(first, left[c - 1] if c else nothing, left[c])
            b = jnp.where(last, right[c + 1] if c + 1 < tiles else nothing, right[c])
            out.append(a + b)
        return out

    def hessian(own, halo):
        side, side_halo = sideways(own), sideways(halo)
        new_own, new_halo = [], []
        for c in range(tiles):
            own_dn, halo_dn = pltpu.roll(own[c], 1, 0), pltpu.roll(halo[c], 1, 0)
            own_up, halo_up = pltpu.roll(own[c], 7, 0), pltpu.roll(halo[c], 7, 0)
            beside = side[c] + jnp.where(top, halo_dn, own_dn) + jnp.where(bottom, halo_up, own_up)
            new_own.append(dd_ref[:, at(c)] * own[c] - beside)
            beside = side_halo[c] + jnp.where(top, own_dn, halo_dn) + jnp.where(bottom, own_up, halo_up)
            new_halo.append(valid * (dd_halo_ref[:, at(c)] * halo[c] - beside))
        return new_own, new_halo

    def inner(a, b):
        total = a[0] * b[0]
        for c in range(1, tiles):
            total = total + a[c] * b[c]
        return total

    def rows(total):
        total = total + pltpu.roll(total, 4, 0)
        total = total + pltpu.roll(total, 2, 0)
        return total + pltpu.roll(total, 1, 0)

    def one(p, carry):
        halo_ref[0:4, :] = up_ref[p]
        halo_ref[5:8, :] = dn_ref[p]
        own = [2.0 * signs_ref[p, :, at(c)].astype(jnp.float32) - 1.0 for c in range(tiles)]
        halo = [halo_ref[:, at(c)] for c in range(tiles)]
        sums = []
        for out in (v1_ref, v2_ref, v3_ref):
            new_own, new_halo = hessian(own, halo)
            for c in range(tiles):
                out[p, :, at(c)] = new_own[c]
            sums += [inner(own, new_own), inner(new_own, new_own)]
            own, halo = new_own, new_halo
        side = sideways(own)
        quad = nothing
        for c in range(tiles):
            below = jnp.where(bottom, pltpu.roll(halo[c], 7, 0), pltpu.roll(own[c], 7, 0))
            quad = quad + own[c] * (dd_ref[:, at(c)] * own[c] - side[c] - 2.0 * below)
        sums.append(quad)
        packed = nothing
        for k, total in enumerate(sums):
            packed = jnp.where(sub == k, rows(total), packed)
        part_ref[pl.ds(pl.multiple_of((step * BLOCK + p) * 8, 8), 8), :] = packed
        return carry

    lax.fori_loop(0, BLOCK, one, 0)

    @pl.when(step == pl.num_programs(0) - 1)
    def _():
        ones = jnp.ones((sums_ref.shape[0], LANES), jnp.float32)
        sums_ref[...] = lax.dot_general(
            ones, part_ref[...], (((1,), (1,)), ((), ())),
            precision=lax.Precision.HIGHEST, preferred_element_type=jnp.float32,
        )


def coefficients(mu, shift):
    zero = jnp.zeros_like(mu[0])
    moved = [mu[k + 1] + shift * mu[k] for k in range(2 * ITERS - 1)]

    def quadratic(c, moments):
        total = None
        n = len(c)
        for s in range(2 * n - 1):
            pairs = [c[a] * c[s - a] for a in range(max(0, s - n + 1), min(n, s + 1))]
            term = functools.reduce(lambda a, b: a + b, pairs) * moments[s]
            total = term if total is None else total + term
        return total

    residual = [jnp.ones_like(mu[0])]
    direction = residual
    solution = [zero] * ITERS
    norm_now = mu[0]
    for i in range(ITERS):
        step = norm_now / quadratic(direction, moved)
        solution = [x + step * direction[k] if k <= i else x for k, x in enumerate(solution)]
        if i + 1 < ITERS:
            applied = [shift * d for d in direction] + [zero]
            applied = [a + (direction[k - 1] if k else zero) for k, a in enumerate(applied)]
            residual = [r - step * a for r, a in zip(residual + [zero], applied)]
            norm_next = quadratic(residual, mu)
            ratio = norm_next / norm_now
            direction = [r + ratio * d for r, d in zip(residual, direction + [zero])]
            norm_now = norm_next
    return solution


def solve_kernel(cells, sums_ref, coef_ref, trace_ref):
    row = jnp.sum(sums_ref[...], axis=0, keepdims=True)
    width = row.shape[1]
    row = jnp.broadcast_to(row, (8, width))
    lane = lax.broadcasted_iota(jnp.int32, (8, width), 1)
    mu = [jnp.full((8, width), cells, jnp.float32), row]
    mu += [pltpu.roll(row, width - k, 1) for k in range(1, 2 * ITERS - 1)]
    coef = coefficients(mu, SHIFT)
    packed = jnp.zeros((8, width), jnp.float32)
    trace = jnp.zeros((8, width), jnp.float32)
    for k in range(ITERS):
        packed = jnp.where(lane % 8 == k, pltpu.roll(coef[k], k, 1) if k else coef[k], packed)
        trace = trace + coef[k] * mu[k]
    trace = jnp.where(lane % 8 == 0, trace, 0.0)
    total = jnp.sum(trace, axis=1, keepdims=True)
    trace_ref[...] = jnp.broadcast_to(total, trace_ref.shape)
    across = jnp.transpose(packed)
    coef_ref[...] = jnp.broadcast_to(across[:, 0:1], coef_ref.shape)


def combine_kernel(coef_ref, signs_ref, v1_ref, v2_ref, v3_ref, out_ref):
    step = pl.program_id(0)
    tiles = out_ref.shape[2] // LANES

    def one(p, carry):
        base = (step * BLOCK + p) * 8
        c = [coef_ref[pl.ds(base + k, 1), :] for k in range(ITERS)]
        for t in range(tiles):
            at = pl.ds(t * LANES, LANES)
            probe = 2.0 * signs_ref[p, :, at].astype(jnp.float32) - 1.0
            out_ref[p, :, at] = (
                c[0] * probe + c[1] * v1_ref[p, :, at] + c[2] * v2_ref[p, :, at] + c[3] * v3_ref[p, :, at]
            )
        return carry

    lax.fori_loop(0, BLOCK, one, 0)


def on_device(probe_signs, sensor_mask, sensor_weight, prior_mass):
    probes, rows, columns = probe_signs.shape
    strips = lax.axis_size("space")
    groups = lax.axis_size("probe")
    me = lax.axis_index("space")
    dd = sensor_mask.astype(jnp.float32) * sensor_weight + prior_mass + (4.0 - SHIFT)

    def edge(begin, end):
        signs = 2.0 * probe_signs[:, begin:end].astype(jnp.float32) - 1.0
        return jnp.concatenate([signs, dd[None, begin:end]], axis=0)

    from_above = lax.ppermute(edge(rows - 3, rows), "space", [(i, i + 1) for i in range(strips - 1)])
    from_below = lax.ppermute(edge(0, 4), "space", [(i + 1, i) for i in range(strips - 1)])
    sub = lax.broadcasted_iota(jnp.int32, (8, LANES), 0)
    outside = jnp.where(sub < 4, me == strips - 1, me == 0)
    valid = jnp.where(outside, 0.0, 1.0).astype(jnp.float32)

    steps = probes // BLOCK
    block = pl.BlockSpec((BLOCK, rows, columns), lambda i: (i, 0, 0))
    field = jax.ShapeDtypeStruct(probe_signs.shape, jnp.float32)
    v1, v2, v3, sums = pl.pallas_call(
        powers_kernel,
        grid=(steps,),
        in_specs=[
            block,
            pl.BlockSpec((rows, columns), lambda i: (0, 0)),
            pl.BlockSpec((BLOCK, 4, columns), lambda i: (i, 0, 0)),
            pl.BlockSpec((1, 4, columns), lambda i: (probes, 0, 0)),
            pl.BlockSpec((BLOCK, 3, columns), lambda i: (i, 0, 0)),
            pl.BlockSpec((1, 3, columns), lambda i: (probes, 0, 0)),
            pl.BlockSpec((8, LANES), lambda i: (0, 0)),
        ],
        out_specs=[block, block, block, pl.BlockSpec((strips, probes * 8), lambda i: (0, 0))],
        out_shape=[field, field, field, jax.ShapeDtypeStruct((strips, probes * 8), jnp.float32)],
        scratch_shapes=[
            pltpu.VMEM((8, columns), jnp.float32),
            pltpu.VMEM((8, columns), jnp.float32),
            pltpu.VMEM((probes * 8, LANES), jnp.float32),
        ],
    )(probe_signs, dd, from_below, from_below, from_above, from_above, valid)

    sums = lax.all_to_all(sums, "space", split_axis=0, concat_axis=0, tiled=True)

    cells = float(rows * strips * columns)
    coef, trace = pl.pallas_call(
        functools.partial(solve_kernel, cells),
        out_shape=[
            jax.ShapeDtypeStruct((probes * 8, LANES), jnp.float32),
            jax.ShapeDtypeStruct((8, LANES), jnp.float32),
        ],
    )(sums)

    trace = trace[0, 0]
    others = [
        lax.ppermute(trace, "probe", [(i, (i + k) % groups) for i in range(groups)])
        for k in range(1, groups)
    ]

    solution = pl.pallas_call(
        combine_kernel,
        grid=(steps,),
        in_specs=[pl.BlockSpec((probes * 8, LANES), lambda i: (0, 0)), block, block, block, block],
        out_specs=block,
        out_shape=field,
        cost_estimate=pl.CostEstimate(flops=8 * probes * rows * columns, bytes_accessed=20 * probes * rows * columns, transcendentals=0),
    )(coef, probe_signs, v1, v2, v3)

    rank = lax.axis_index("probe")
    everyone = jnp.stack([trace] + others)
    ordered = jnp.stack([everyone[(rank - g) % groups] for g in range(groups)])
    trace_sum = jnp.sum(ordered)
    return solution, trace_sum / (float(probes * groups) * cells)


def solution(mesh):
    return jax.shard_map(
        on_device,
        mesh=mesh,
        in_specs=(P("probe", "space", None), P("space", None), P("space", None), P("space", None)),
        out_specs=(P("probe", "space", None), P()),
        check_vma=False,
    )
```

```python
import functools

import jax
import jax.numpy as jnp
from jax import lax
from jax.experimental import pallas as pl
from jax.experimental.pallas import tpu as pltpu
from jax.sharding import PartitionSpec as P


ITERS = 4
SHIFT = 9.0
LANES = 128
GROUP = 8
CHUNKS = 2
AMPLIFIED = 600.0
VMEM_LIMIT = 16 * 1024 * 1024


VMEM = pl.BlockSpec(memory_space=pltpu.VMEM)
HBM = pl.BlockSpec(memory_space=pltpu.HBM)


def operate(vector, diagonal):
    strips = lax.axis_size("space")
    above = lax.ppermute(vector[:, -1:], "space", [(i, i + 1) for i in range(strips - 1)])
    below = lax.ppermute(vector[:, :1], "space", [(i + 1, i) for i in range(strips - 1)])
    padded = jnp.pad(jnp.concatenate([above, vector, below], axis=1), ((0, 0), (0, 0), (1, 1)))
    beside = padded[:, 2:, 1:-1] + padded[:, :-2, 1:-1]
    beside = beside + padded[:, 1:-1, 2:] + padded[:, 1:-1, :-2]
    return (4.0 + diagonal) * vector - beside


def of_everyone(values, axis):
    copies = jnp.broadcast_to(values, (lax.axis_size(axis), *values.shape))
    return jnp.sum(lax.all_to_all(copies, axis, split_axis=0, concat_axis=0, tiled=True), axis=0)


def per_probe(values):
    return of_everyone(jnp.sum(values, axis=(1, 2)), "space")


def iterate_on_device(probe_signs, diagonal):
    probes = 2.0 * probe_signs.astype(jnp.float32) - 1.0

    def iteration(_, state):
        solution, residual, direction, norm_now = state
        applied = operate(direction, diagonal)
        step = (norm_now / per_probe(direction * applied))[:, None, None]
        solution = solution + step * direction
        residual = residual - step * applied
        norm_next = per_probe(residual * residual)
        direction = residual + (norm_next / norm_now)[:, None, None] * direction
        return solution, residual, direction, norm_next

    cells = probes.shape[1] * lax.axis_size("space") * probes.shape[2]
    norm_now = jnp.full((probes.shape[0],), float(cells), jnp.float32)
    solution = lax.fori_loop(0, ITERS, iteration, (jnp.zeros_like(probes), probes, probes, norm_now))[0]
    quadratics = per_probe(probes * solution)
    trace_sum = of_everyone(jnp.sum(quadratics)[None], "probe")[0]
    return solution, trace_sum / float(probes.shape[0] * lax.axis_size("probe") * cells)


def edge_of(r, refs):
    up_ref, mid_ref, dn_ref = refs
    return (up_ref, r) if r < 4 else (mid_ref, 0) if r == 4 else (dn_ref, r - 5)


def prepare_kernel(signs_hbm, mask_hbm, weight_hbm, mass_hbm, *refs):
    outs = [refs[3 * n : 3 * n + 3] for n in range(CHUNKS)]
    signs_ref, mask_ref, weight_ref, mass_ref, sems = refs[3 * CHUNKS :]
    probes, rows, columns = signs_ref.shape
    count = probes // CHUNKS
    groups = probes // GROUP
    fields = [(mask_hbm, mask_ref), (weight_hbm, weight_ref), (mass_hbm, mass_ref)]
    copies = []
    for g in range(groups):
        mine = pl.ds(g * GROUP, GROUP)
        copies.append(pltpu.make_async_copy(signs_hbm.at[mine], signs_ref.at[mine], sems.at[g]))
    for n, (src, dst) in enumerate(fields):
        copies.append(pltpu.make_async_copy(src, dst, sems.at[groups + n]))
    for copy in copies:
        copy.start()
    for g in range(groups):
        copies[g].wait()
        refs = outs[g * GROUP // count]
        base = g * GROUP % count
        for c in range(columns // LANES):
            at = slice(c * LANES, (c + 1) * LANES)
            block = 2.0 * signs_ref[g * GROUP : (g + 1) * GROUP, :, at].astype(jnp.float32) - 1.0
            block = jnp.swapaxes(block, 0, 1)
            for r in range(rows):
                ref, start = edge_of(r, refs)
                ref[start * count + base : start * count + base + GROUP, at] = block[r]
    for copy in copies[groups:]:
        copy.wait()
    diagonal = mask_ref[...].astype(jnp.float32) * weight_ref[...] + mass_ref[...]
    outs[0][0][4 * count :, :] = diagonal
    outs[0][2][3 * count :, :] = diagonal


def powers_kernel(chunk, *refs):
    up_ref, mid_ref, dn_ref, below_ref, above_ref = refs[:5]
    if chunk:
        up_dd_ref, below_dd_ref, above_dd_ref, earlier_ref = refs[5:9]
        v1_ref, v2_ref, v3_ref, sums_ref, dd_ref, h1_ref, h2_ref, h3_ref, total_ref, part_ref = refs[9:]
    else:
        up_dd_ref, below_dd_ref, above_dd_ref = up_ref, below_ref, above_ref
        v1_ref, v2_ref, v3_ref, part_ref, dd_ref, h1_ref, h2_ref, h3_ref = refs[5:]
    rows, probes, columns = v1_ref.shape
    tiles = columns // LANES
    lane = lax.broadcasted_iota(jnp.int32, (GROUP, LANES), 1)
    first, last = lane == 0, lane == LANES - 1
    nothing = jnp.zeros((GROUP, LANES), jnp.float32)

    def at(c):
        return pl.ds(c * LANES, LANES)

    def spread(ref, row, to):
        line = ref[row : row + 1, :]
        dd_ref[to] = jnp.broadcast_to(line + (4.0 - SHIFT), (GROUP, columns))
        return jnp.where(jnp.broadcast_to(line[:, :LANES], (GROUP, LANES)) > 0.0, 1.0, 0.0)

    spread(above_dd_ref, 3 * probes + 6, 0)
    in_above = spread(above_dd_ref, 3 * probes + 7, 1)
    for r in range(rows):
        spread(up_dd_ref, 4 * probes + r, r + 2)
    in_below = spread(below_dd_ref, 4 * probes, 10)
    spread(below_dd_ref, 4 * probes + 1, 11)
    spread(below_dd_ref, 4 * probes + 2, 12)
    part_ref[7 * probes :, :] = jnp.zeros((probes, LANES), jnp.float32)

    own = [None, v1_ref, v2_ref, v3_ref]
    halo = [None, h1_ref, h2_ref, h3_ref]
    place = [None, {-2: 0, -1: 1, 8: 2, 9: 3, 10: 4}, {-1: 0, 8: 1, 9: 2}, {8: 0}]

    def where(level, r, base):
        if level:
            if 0 <= r < rows:
                return own[level], (r, pl.ds(base, GROUP))
            return halo[level], (place[level][r], slice(None))
        if r < 0:
            return above_ref, (pl.ds((r + 3) * probes + base, GROUP),)
        if r < 4:
            return up_ref, (pl.ds(r * probes + base, GROUP),)
        if r == 4:
            return mid_ref, (pl.ds(base, GROUP),)
        if r < rows:
            return dn_ref, (pl.ds((r - 5) * probes + base, GROUP),)
        return below_ref, (pl.ds((r - rows) * probes + base, GROUP),)

    def sideways(v):
        left = [pltpu.roll(t, 1, 1) for t in v]
        right = [pltpu.roll(t, LANES - 1, 1) for t in v]
        out = []
        for c in range(tiles):
            a = jnp.where(first, left[c - 1] if c else nothing, left[c])
            b = jnp.where(last, right[c + 1] if c + 1 < tiles else nothing, right[c])
            out.append(a + b)
        return out

    def group(g, carry):
        base = pl.multiple_of(g * GROUP, GROUP)

        def line(level, r):
            ref, index = where(level, r, base)
            return [ref[index + (at(c),)] for c in range(tiles)]

        totals = []
        for level, (begin, end) in enumerate([(-2, 11), (-1, 10), (0, 9)]):
            cross, square = nothing, nothing
            before, here = line(level, begin - 1), line(level, begin)
            for r in range(begin, end):
                after = line(level, r + 1)
                side = sideways(here)
                ref, index = where(level + 1, r, base)
                for c in range(tiles):
                    value = dd_ref[r + 2, :, at(c)] * here[c] - (side[c] + (before[c] + after[c]))
                    if r < 0:
                        value = in_above * value
                    if r >= rows:
                        value = in_below * value
                    ref[index + (at(c),)] = value
                    if 0 <= r < rows:
                        cross = cross + here[c] * value
                        square = square + value * value
                before, here = here, after
            totals += [cross, square]
        quad = nothing
        here = line(3, 0)
        for r in range(rows):
            after = line(3, r + 1)
            side = sideways(here)
            for c in range(tiles):
                quad = quad + here[c] * (dd_ref[r + 2, :, at(c)] * here[c] - (side[c] + (after[c] + after[c])))
            here = after
        totals.append(quad)
        for k, total in enumerate(totals):
            part_ref[pl.ds(k * probes + base, GROUP), :] = total
        return carry

    lax.fori_loop(0, probes // GROUP, group, 0)
    if not chunk:
        return
    for k in range(8):
        begin = k * CHUNKS * probes
        total_ref[begin : begin + probes, :] = earlier_ref[k * probes : (k + 1) * probes, :]
        total_ref[begin + probes : begin + 2 * probes, :] = part_ref[k * probes : (k + 1) * probes, :]
    ones = jnp.ones((GROUP, LANES), jnp.float32)
    line = lax.dot_general(
        ones, total_ref[...], (((1,), (1,)), ((), ())),
        precision=lax.Precision.HIGHEST, preferred_element_type=jnp.float32,
    )
    sums_ref[...] = jnp.broadcast_to(line[None, 0:1, :], sums_ref.shape)


def quadratic(c, moments):
    total = None
    n = len(c)
    for s in range(2 * n - 1):
        pairs = [c[a] * c[s - a] for a in range(max(0, s - n + 1), min(n, s + 1))]
        term = functools.reduce(lambda a, b: a + b, pairs) * moments[s]
        total = term if total is None else total + term
    return total


def coefficients(mu, shift):
    zero = jnp.zeros_like(mu[0])
    size = [jnp.abs(m) for m in mu]
    moved = [mu[k + 1] + shift * mu[k] for k in range(2 * ITERS - 1)]
    moved_size = [size[k + 1] + shift * size[k] for k in range(2 * ITERS - 1)]
    residual = [jnp.ones_like(mu[0])]
    direction = residual
    solution = [zero] * ITERS
    norm_now = mu[0]
    lost = jnp.ones_like(mu[0])
    amplified = zero
    for i in range(ITERS):
        curvature = quadratic(direction, moved)
        step = norm_now / curvature
        loss = quadratic([jnp.abs(d) for d in direction], moved_size) / jnp.abs(curvature)
        length = jnp.sqrt(jnp.abs(quadratic(direction, mu)))
        amplified = amplified + (loss + lost) * (jnp.abs(step) * length)
        solution = [x + step * direction[k] if k <= i else x for k, x in enumerate(solution)]
        if i + 1 < ITERS:
            applied = [shift * d for d in direction] + [zero]
            applied = [a + (direction[k - 1] if k else zero) for k, a in enumerate(applied)]
            residual = [r - step * a for r, a in zip(residual + [zero], applied)]
            norm_next = quadratic(residual, mu)
            lost = quadratic([jnp.abs(r) for r in residual], size) / jnp.abs(norm_next)
            ratio = norm_next / norm_now
            direction = [r + ratio * d for r, d in zip(residual, direction + [zero])]
            norm_now = norm_next
    for k in range(ITERS):
        amplified = amplified + jnp.abs(solution[k]) * jnp.sqrt(size[2 * k])
    length = jnp.sqrt(quadratic(solution, mu))
    return solution, amplified / length


def solve_kernel(cells, groups, sums_ref, coef_ref, trace_ref):
    row = jnp.sum(sums_ref[...], axis=0)
    width = row.shape[1]
    probes = width // 8
    row = jnp.broadcast_to(row, (8, width))
    mu = [jnp.full((8, LANES), cells, jnp.float32)]
    for k in range(2 * ITERS - 1):
        moved = pltpu.roll(row, width - k * probes, 1) if k else row
        mu.append(moved[:, :LANES])
    coef, amplified = coefficients(mu, SHIFT)
    sub = lax.broadcasted_iota(jnp.int32, (8, LANES), 0)
    lane = lax.broadcasted_iota(jnp.int32, (8, LANES), 1)
    packed = jnp.zeros((8, LANES), jnp.float32)
    trace = jnp.zeros((8, LANES), jnp.float32)
    for k in range(ITERS):
        packed = jnp.where(sub == k, coef[k], packed)
        trace = trace + coef[k] * mu[k]
    trace = jnp.where(lane < probes, trace, 0.0)
    total = jnp.sum(trace, axis=1, keepdims=True) / (float(probes * groups) * cells)
    unsafe = jnp.where(amplified < AMPLIFIED, 0.0, 1.0)
    unsafe = jnp.max(jnp.where(lane < probes, unsafe, 0.0), axis=1, keepdims=True)
    both = jnp.where(lane < LANES // 2, jnp.broadcast_to(total, lane.shape), jnp.broadcast_to(unsafe, lane.shape))
    trace_ref[...] = jnp.where(lane < LANES - 1, both, 0.0)[0:1]
    across = jnp.transpose(packed)
    for k in range(ITERS):
        coef_ref[k * probes : (k + 1) * probes, :] = jnp.broadcast_to(across[:probes, k : k + 1], (probes, LANES))


def combine_kernel(coef_ref, *refs):
    chunks = [refs[6 * n : 6 * n + 6] for n in range(CHUNKS)]
    out_ref, made_ref, sems = refs[6 * CHUNKS :]
    probes, rows, columns = made_ref.shape
    count = probes // CHUNKS

    def copy(g):
        mine = pl.ds(g * GROUP, GROUP)
        return pltpu.make_async_copy(made_ref.at[mine], out_ref.at[mine], sems.at[g])

    for g in range(probes // GROUP):
        v1_ref, v2_ref, v3_ref = chunks[g * GROUP // count][3:]
        base = g * GROUP
        local = base % count
        mine = slice(local, local + GROUP)
        c = [coef_ref[k * probes + base : k * probes + base + GROUP, :] for k in range(ITERS)]
        for t in range(columns // LANES):
            at = slice(t * LANES, (t + 1) * LANES)
            made = []
            for r in range(rows):
                ref, start = edge_of(r, chunks[base // count][:3])
                probe = ref[start * count + local : start * count + local + GROUP, at]
                made.append(
                    (c[0] * probe + c[1] * v1_ref[r, mine, at]) + (c[2] * v2_ref[r, mine, at] + c[3] * v3_ref[r, mine, at])
                )
            made_ref[base : base + GROUP, :, at] = jnp.swapaxes(jnp.stack(made), 0, 1)
        copy(g).start()
    for g in range(probes // GROUP):
        copy(g).wait()


def on_device(probe_signs, sensor_mask, sensor_weight, prior_mass):
    probes, rows, columns = probe_signs.shape
    strips = lax.axis_size("space")
    groups = lax.axis_size("probe")
    count = probes // CHUNKS
    params = pltpu.CompilerParams(vmem_limit_bytes=VMEM_LIMIT)

    def shaped(*shape):
        return jax.ShapeDtypeStruct(shape, jnp.float32)

    extra = [8] + [0] * (CHUNKS - 1)
    edges = pl.pallas_call(
        prepare_kernel,
        in_specs=[HBM] * 4,
        out_specs=[VMEM] * (3 * CHUNKS),
        out_shape=[shaped(r * count + (e if r > 1 else 0), columns) for e in extra for r in (4, 1, 3)],
        scratch_shapes=[
            pltpu.VMEM((probes, rows, columns), jnp.int32),
            pltpu.VMEM((rows, columns), jnp.int32),
            pltpu.VMEM((rows, columns), jnp.float32),
            pltpu.VMEM((rows, columns), jnp.float32),
            pltpu.SemaphoreType.DMA((probes // GROUP + 3,)),
        ],
        compiler_params=params,
    )(probe_signs, sensor_mask, sensor_weight, prior_mass)
    edges = [edges[3 * n : 3 * n + 3] for n in range(CHUNKS)]

    received = []
    for up, mid, dn in edges:
        below = lax.ppermute(up, "space", [(i + 1, i) for i in range(strips - 1)])
        above = lax.ppermute(dn, "space", [(i, i + 1) for i in range(strips - 1)])
        received.append((below, above))

    field = shaped(rows, count, columns)
    powers = []
    for n, ((up, mid, dn), (below, above)) in enumerate(zip(edges, received)):
        args = [up, mid, dn, below, above]
        sums = shaped(8 * count, LANES)
        scratch = [pltpu.VMEM((size, GROUP, columns), jnp.float32) for size in (rows + 5, 5, 3, 1)]
        if n:
            args += [edges[0][0], *received[0], powers[0][3]]
            sums = shaped(strips, 1, 8 * probes)
            scratch += [pltpu.VMEM((8 * probes, LANES), jnp.float32), pltpu.VMEM((8 * count, LANES), jnp.float32)]
        powers.append(
            pl.pallas_call(
                functools.partial(powers_kernel, n),
                in_specs=[VMEM] * len(args),
                out_specs=[VMEM] * 4,
                out_shape=[field, field, field, sums],
                scratch_shapes=scratch,
                compiler_params=params,
            )(*args)
        )

    sums = lax.all_to_all(powers[-1][3], "space", split_axis=0, concat_axis=0, tiled=True)

    cells = float(rows * strips * columns)
    coef, trace = pl.pallas_call(
        functools.partial(solve_kernel, cells, groups),
        in_specs=[VMEM],
        out_specs=[VMEM, VMEM],
        out_shape=[shaped(ITERS * probes, LANES), shaped(1, LANES)],
        compiler_params=params,
    )(sums)

    one, two, three = [
        lax.ppermute(trace, "probe", [(i, (i + k) % groups) for i in range(groups)])
        for k in range(1, groups)
    ]

    args = [coef]
    for edge, power in zip(edges, powers):
        args += [*edge, *power[:3]]
    combined = pl.pallas_call(
        combine_kernel,
        in_specs=[VMEM] * len(args),
        out_specs=HBM,
        out_shape=shaped(probes, rows, columns),
        scratch_shapes=[
            pltpu.VMEM((probes, rows, columns), jnp.float32),
            pltpu.SemaphoreType.DMA((probes // GROUP,)),
        ],
        compiler_params=params,
        cost_estimate=pl.CostEstimate(
            flops=8 * probes * rows * columns, bytes_accessed=20 * probes * rows * columns, transcendentals=0
        ),
    )(*args)

    everyone = (trace + two) + (one + three)

    def again(state):
        _, turn, _, _ = state
        past = turn.astype(jnp.int32)
        diagonal = (sensor_mask + past).astype(jnp.float32) * sensor_weight + prior_mass
        made, cell = iterate_on_device(probe_signs + past, diagonal)
        return turn, turn + 1.0, made, cell

    state = (everyone[0, LANES // 2], everyone[0, LANES - 1], combined, everyone[0, 0])
    return lax.while_loop(lambda state: state[0] > 0.0, again, state)[2:]


def solution(mesh):
    return jax.shard_map(
        on_device,
        mesh=mesh,
        in_specs=(P("probe", "space", None), P("space", None), P("space", None), P("space", None)),
        out_specs=(P("probe", "space", None), P()),
        check_vma=False,
    )
```

```python
import functools

import jax
import jax.numpy as jnp
from jax import lax
from jax.experimental import pallas as pl
from jax.experimental.pallas import tpu as pltpu
from jax.sharding import PartitionSpec as P


ITERS = 4
SHIFT = 9.0
LANES = 128
GROUP = 8
CHUNKS = 2
AMPLIFIED = 600.0
VMEM_LIMIT = 16 * 1024 * 1024


VMEM = pl.BlockSpec(memory_space=pltpu.VMEM)
HBM = pl.BlockSpec(memory_space=pltpu.HBM)


def operate(vector, diagonal):
    strips = lax.axis_size("space")
    above = lax.ppermute(vector[:, -1:], "space", [(i, i + 1) for i in range(strips - 1)])
    below = lax.ppermute(vector[:, :1], "space", [(i + 1, i) for i in range(strips - 1)])
    padded = jnp.pad(jnp.concatenate([above, vector, below], axis=1), ((0, 0), (0, 0), (1, 1)))
    beside = padded[:, 2:, 1:-1] + padded[:, :-2, 1:-1]
    beside = beside + padded[:, 1:-1, 2:] + padded[:, 1:-1, :-2]
    return (4.0 + diagonal) * vector - beside


def of_everyone(values, axis):
    copies = jnp.broadcast_to(values, (lax.axis_size(axis), *values.shape))
    return jnp.sum(lax.all_to_all(copies, axis, split_axis=0, concat_axis=0, tiled=True), axis=0)


def per_probe(values):
    return of_everyone(jnp.sum(values, axis=(1, 2)), "space")


def iterate_on_device(probe_signs, diagonal):
    probes = 2.0 * probe_signs.astype(jnp.float32) - 1.0

    def iteration(_, state):
        solution, residual, direction, norm_now = state
        applied = operate(direction, diagonal)
        step = (norm_now / per_probe(direction * applied))[:, None, None]
        solution = solution + step * direction
        residual = residual - step * applied
        norm_next = per_probe(residual * residual)
        direction = residual + (norm_next / norm_now)[:, None, None] * direction
        return solution, residual, direction, norm_next

    cells = probes.shape[1] * lax.axis_size("space") * probes.shape[2]
    norm_now = jnp.full((probes.shape[0],), float(cells), jnp.float32)
    solution = lax.fori_loop(0, ITERS, iteration, (jnp.zeros_like(probes), probes, probes, norm_now))[0]
    quadratics = per_probe(probes * solution)
    trace_sum = of_everyone(jnp.sum(quadratics)[None], "probe")[0]
    return solution, trace_sum / float(probes.shape[0] * lax.axis_size("probe") * cells)


def edge_of(r, n, count, refs):
    up_ref, mid_ref, *dn_refs = refs
    if r < 4:
        return up_ref, (r * CHUNKS + n) * count
    if r == 4:
        return mid_ref, n * count
    return dn_refs[n], (r - 5) * count


def prepare_kernel(signs_hbm, mask_hbm, weight_hbm, mass_hbm, *refs):
    outs = refs[: CHUNKS + 2]
    signs_ref, mask_ref, weight_ref, mass_ref, sems = refs[CHUNKS + 2 :]
    probes, rows, columns = signs_ref.shape
    count = probes // CHUNKS
    groups = probes // GROUP
    fields = [(mask_hbm, mask_ref), (weight_hbm, weight_ref), (mass_hbm, mass_ref)]
    copies = []
    for g in range(groups):
        mine = pl.ds(g * GROUP, GROUP)
        copies.append(pltpu.make_async_copy(signs_hbm.at[mine], signs_ref.at[mine], sems.at[g]))
    for n, (src, dst) in enumerate(fields):
        copies.append(pltpu.make_async_copy(src, dst, sems.at[groups + n]))
    for copy in copies:
        copy.start()
    for g in range(groups):
        copies[g].wait()
        chunk, base = divmod(g * GROUP, count)
        for c in range(columns // LANES):
            at = slice(c * LANES, (c + 1) * LANES)
            block = 2.0 * signs_ref[g * GROUP : (g + 1) * GROUP, :, at].astype(jnp.float32) - 1.0
            block = jnp.swapaxes(block, 0, 1)
            for r in range(rows):
                ref, start = edge_of(r, chunk, count, outs)
                ref[start + base : start + base + GROUP, at] = block[r]
    for copy in copies[groups:]:
        copy.wait()
    diagonal = mask_ref[...].astype(jnp.float32) * weight_ref[...] + mass_ref[...]
    outs[0][4 * probes :, :] = diagonal
    outs[2][3 * count :, :] = diagonal


def powers_kernel(chunk, *refs):
    up_ref, mid_ref, below_ref, dn_ref, above_ref = refs[:5]
    if chunk:
        above_dd_ref, earlier_ref = refs[5:7]
        v1_ref, v2_ref, v3_ref, sums_ref, dd_ref, h1_ref, h2_ref, h3_ref, total_ref, part_ref = refs[7:]
    else:
        above_dd_ref = above_ref
        v1_ref, v2_ref, v3_ref, part_ref, dd_ref, h1_ref, h2_ref, h3_ref = refs[5:]
    rows, probes, columns = v1_ref.shape
    tiles = columns // LANES
    lane = lax.broadcasted_iota(jnp.int32, (GROUP, LANES), 1)
    first, last = lane == 0, lane == LANES - 1
    nothing = jnp.zeros((GROUP, LANES), jnp.float32)

    def at(c):
        return pl.ds(c * LANES, LANES)

    def spread(ref, row, to):
        line = ref[row : row + 1, :]
        dd_ref[to] = jnp.broadcast_to(line + (4.0 - SHIFT), (GROUP, columns))
        return jnp.where(jnp.broadcast_to(line[:, :LANES], (GROUP, LANES)) > 0.0, 1.0, 0.0)

    spread(above_dd_ref, 3 * probes + 6, 0)
    in_above = spread(above_dd_ref, 3 * probes + 7, 1)
    for r in range(rows):
        spread(up_ref, 4 * CHUNKS * probes + r, r + 2)
    in_below = spread(below_ref, 4 * CHUNKS * probes, 10)
    spread(below_ref, 4 * CHUNKS * probes + 1, 11)
    spread(below_ref, 4 * CHUNKS * probes + 2, 12)
    part_ref[7 * probes :, :] = jnp.zeros((probes, LANES), jnp.float32)

    own = [None, v1_ref, v2_ref, v3_ref]
    halo = [None, h1_ref, h2_ref, h3_ref]
    place = [None, {-2: 0, -1: 1, 8: 2, 9: 3, 10: 4}, {-1: 0, 8: 1, 9: 2}, {8: 0}]

    def where(level, r, base):
        if level:
            if 0 <= r < rows:
                return own[level], (r, pl.ds(base, GROUP))
            return halo[level], (place[level][r], slice(None))
        if r < 0:
            return above_ref, (pl.ds((r + 3) * probes + base, GROUP),)
        if r < 4:
            return up_ref, (pl.ds((r * CHUNKS + chunk) * probes + base, GROUP),)
        if r == 4:
            return mid_ref, (pl.ds(chunk * probes + base, GROUP),)
        if r < rows:
            return dn_ref, (pl.ds((r - 5) * probes + base, GROUP),)
        return below_ref, (pl.ds(((r - rows) * CHUNKS + chunk) * probes + base, GROUP),)

    def sideways(v):
        left = [pltpu.roll(t, 1, 1) for t in v]
        right = [pltpu.roll(t, LANES - 1, 1) for t in v]
        out = []
        for c in range(tiles):
            a = jnp.where(first, left[c - 1] if c else nothing, left[c])
            b = jnp.where(last, right[c + 1] if c + 1 < tiles else nothing, right[c])
            out.append(a + b)
        return out

    def group(g, carry):
        base = pl.multiple_of(g * GROUP, GROUP)

        def line(level, r):
            ref, index = where(level, r, base)
            return [ref[index + (at(c),)] for c in range(tiles)]

        totals = []
        for level, (begin, end) in enumerate([(-2, 11), (-1, 10), (0, 9)]):
            cross, square = nothing, nothing
            before, here = line(level, begin - 1), line(level, begin)
            for r in range(begin, end):
                after = line(level, r + 1)
                side = sideways(here)
                ref, index = where(level + 1, r, base)
                for c in range(tiles):
                    value = dd_ref[r + 2, :, at(c)] * here[c] - (side[c] + (before[c] + after[c]))
                    if r < 0:
                        value = in_above * value
                    if r >= rows:
                        value = in_below * value
                    ref[index + (at(c),)] = value
                    if 0 <= r < rows:
                        cross = cross + here[c] * value
                        square = square + value * value
                before, here = here, after
            totals += [cross, square]
        quad = nothing
        here = line(3, 0)
        for r in range(rows):
            after = line(3, r + 1)
            side = sideways(here)
            for c in range(tiles):
                quad = quad + here[c] * (dd_ref[r + 2, :, at(c)] * here[c] - (side[c] + (after[c] + after[c])))
            here = after
        totals.append(quad)
        for k, total in enumerate(totals):
            part_ref[pl.ds(k * probes + base, GROUP), :] = total
        return carry

    lax.fori_loop(0, probes // GROUP, group, 0)
    if not chunk:
        return
    for k in range(8):
        begin = k * CHUNKS * probes
        total_ref[begin : begin + probes, :] = earlier_ref[k * probes : (k + 1) * probes, :]
        total_ref[begin + probes : begin + 2 * probes, :] = part_ref[k * probes : (k + 1) * probes, :]
    ones = jnp.ones((GROUP, LANES), jnp.float32)
    line = lax.dot_general(
        ones, total_ref[...], (((1,), (1,)), ((), ())),
        precision=lax.Precision.HIGHEST, preferred_element_type=jnp.float32,
    )
    sums_ref[...] = jnp.broadcast_to(line[None, 0:1, :], sums_ref.shape)


def quadratic(c, moments):
    total = None
    n = len(c)
    for s in range(2 * n - 1):
        pairs = [c[a] * c[s - a] for a in range(max(0, s - n + 1), min(n, s + 1))]
        term = functools.reduce(lambda a, b: a + b, pairs) * moments[s]
        total = term if total is None else total + term
    return total


def coefficients(mu, shift):
    zero = jnp.zeros_like(mu[0])
    size = [jnp.abs(m) for m in mu]
    moved = [mu[k + 1] + shift * mu[k] for k in range(2 * ITERS - 1)]
    moved_size = [size[k + 1] + shift * size[k] for k in range(2 * ITERS - 1)]
    residual = [jnp.ones_like(mu[0])]
    direction = residual
    solution = [zero] * ITERS
    norm_now = mu[0]
    lost = jnp.ones_like(mu[0])
    amplified = zero
    for i in range(ITERS):
        curvature = quadratic(direction, moved)
        step = norm_now / curvature
        loss = quadratic([jnp.abs(d) for d in direction], moved_size) / jnp.abs(curvature)
        length = jnp.sqrt(jnp.abs(quadratic(direction, mu)))
        amplified = amplified + (loss + lost) * (jnp.abs(step) * length)
        solution = [x + step * direction[k] if k <= i else x for k, x in enumerate(solution)]
        if i + 1 < ITERS:
            applied = [shift * d for d in direction] + [zero]
            applied = [a + (direction[k - 1] if k else zero) for k, a in enumerate(applied)]
            residual = [r - step * a for r, a in zip(residual + [zero], applied)]
            norm_next = quadratic(residual, mu)
            lost = quadratic([jnp.abs(r) for r in residual], size) / jnp.abs(norm_next)
            ratio = norm_next / norm_now
            direction = [r + ratio * d for r, d in zip(residual, direction + [zero])]
            norm_now = norm_next
    for k in range(ITERS):
        amplified = amplified + jnp.abs(solution[k]) * jnp.sqrt(size[2 * k])
    length = jnp.sqrt(quadratic(solution, mu))
    return solution, amplified / length


def solve_kernel(cells, groups, sums_ref, coef_ref, trace_ref):
    row = jnp.sum(sums_ref[...], axis=0)
    width = row.shape[1]
    probes = width // 8
    row = jnp.broadcast_to(row, (8, width))
    mu = [jnp.full((8, LANES), cells, jnp.float32)]
    for k in range(2 * ITERS - 1):
        moved = pltpu.roll(row, width - k * probes, 1) if k else row
        mu.append(moved[:, :LANES])
    coef, amplified = coefficients(mu, SHIFT)
    sub = lax.broadcasted_iota(jnp.int32, (8, LANES), 0)
    lane = lax.broadcasted_iota(jnp.int32, (8, LANES), 1)
    packed = jnp.zeros((8, LANES), jnp.float32)
    trace = jnp.zeros((8, LANES), jnp.float32)
    for k in range(ITERS):
        packed = jnp.where(sub == k, coef[k], packed)
        trace = trace + coef[k] * mu[k]
    trace = jnp.where(lane < probes, trace, 0.0)
    total = jnp.sum(trace, axis=1, keepdims=True) / (float(probes * groups) * cells)
    unsafe = jnp.where(amplified < AMPLIFIED, 0.0, 1.0)
    unsafe = jnp.max(jnp.where(lane < probes, unsafe, 0.0), axis=1, keepdims=True)
    both = jnp.where(lane < LANES // 2, jnp.broadcast_to(total, lane.shape), jnp.broadcast_to(unsafe, lane.shape))
    trace_ref[...] = jnp.where(lane < LANES - 1, both, 0.0)[0:1]
    across = jnp.transpose(packed)
    for k in range(ITERS):
        coef_ref[k * probes : (k + 1) * probes, :] = jnp.broadcast_to(across[:probes, k : k + 1], (probes, LANES))


def combine_kernel(coef_ref, *refs):
    edges = refs[: CHUNKS + 2]
    powers = [refs[CHUNKS + 2 + 3 * n : CHUNKS + 5 + 3 * n] for n in range(CHUNKS)]
    out_ref, made_ref, sems = refs[4 * CHUNKS + 2 :]
    probes, rows, columns = made_ref.shape
    count = probes // CHUNKS

    def copy(g):
        mine = pl.ds(g * GROUP, GROUP)
        return pltpu.make_async_copy(made_ref.at[mine], out_ref.at[mine], sems.at[g])

    for g in range(probes // GROUP):
        base = g * GROUP
        chunk, local = divmod(base, count)
        v1_ref, v2_ref, v3_ref = powers[chunk]
        mine = slice(local, local + GROUP)
        c = [coef_ref[k * probes + base : k * probes + base + GROUP, :] for k in range(ITERS)]
        for t in range(columns // LANES):
            at = slice(t * LANES, (t + 1) * LANES)
            made = []
            for r in range(rows):
                ref, start = edge_of(r, chunk, count, edges)
                probe = ref[start + local : start + local + GROUP, at]
                made.append(
                    (c[0] * probe + c[1] * v1_ref[r, mine, at]) + (c[2] * v2_ref[r, mine, at] + c[3] * v3_ref[r, mine, at])
                )
            made_ref[base : base + GROUP, :, at] = jnp.swapaxes(jnp.stack(made), 0, 1)
        copy(g).start()
    for g in range(probes // GROUP):
        copy(g).wait()


def on_device(probe_signs, sensor_mask, sensor_weight, prior_mass):
    probes, rows, columns = probe_signs.shape
    strips = lax.axis_size("space")
    groups = lax.axis_size("probe")
    count = probes // CHUNKS
    params = pltpu.CompilerParams(vmem_limit_bytes=VMEM_LIMIT)

    def shaped(*shape):
        return jax.ShapeDtypeStruct(shape, jnp.float32)

    edges = pl.pallas_call(
        prepare_kernel,
        in_specs=[HBM] * 4,
        out_specs=[VMEM] * (CHUNKS + 2),
        out_shape=[shaped(4 * probes + rows, columns), shaped(probes, columns)]
        + [shaped(3 * count + (0 if n else rows), columns) for n in range(CHUNKS)],
        scratch_shapes=[
            pltpu.VMEM((probes, rows, columns), jnp.int32),
            pltpu.VMEM((rows, columns), jnp.int32),
            pltpu.VMEM((rows, columns), jnp.float32),
            pltpu.VMEM((rows, columns), jnp.float32),
            pltpu.SemaphoreType.DMA((probes // GROUP + 3,)),
        ],
        compiler_params=params,
    )(probe_signs, sensor_mask, sensor_weight, prior_mass)
    up, mid, *downs = edges
    below = lax.ppermute(up, "space", [(i + 1, i) for i in range(strips - 1)])
    above = []
    for dn in downs:
        above.append(lax.ppermute(dn, "space", [(i, i + 1) for i in range(strips - 1)]))

    field = shaped(rows, count, columns)
    powers = []
    for n in range(CHUNKS):
        args = [up, mid, below, downs[n], above[n]]
        sums = shaped(8 * count, LANES)
        scratch = [pltpu.VMEM((size, GROUP, columns), jnp.float32) for size in (rows + 5, 5, 3, 1)]
        if n:
            args += [above[0], powers[0][3]]
            sums = shaped(strips, 1, 8 * probes)
            scratch += [pltpu.VMEM((8 * probes, LANES), jnp.float32), pltpu.VMEM((8 * count, LANES), jnp.float32)]
        powers.append(
            pl.pallas_call(
                functools.partial(powers_kernel, n),
                in_specs=[VMEM] * len(args),
                out_specs=[VMEM] * 4,
                out_shape=[field, field, field, sums],
                scratch_shapes=scratch,
                compiler_params=params,
            )(*args)
        )

    sums = lax.all_to_all(powers[-1][3], "space", split_axis=0, concat_axis=0, tiled=True)

    cells = float(rows * strips * columns)
    coef, trace = pl.pallas_call(
        functools.partial(solve_kernel, cells, groups),
        in_specs=[VMEM],
        out_specs=[VMEM, VMEM],
        out_shape=[shaped(ITERS * probes, LANES), shaped(1, LANES)],
        compiler_params=params,
    )(sums)

    one, two, three = [
        lax.ppermute(trace, "probe", [(i, (i + k) % groups) for i in range(groups)])
        for k in range(1, groups)
    ]

    args = [coef, *edges]
    for power in powers:
        args += power[:3]
    combined = pl.pallas_call(
        combine_kernel,
        in_specs=[VMEM] * len(args),
        out_specs=HBM,
        out_shape=shaped(probes, rows, columns),
        scratch_shapes=[
            pltpu.VMEM((probes, rows, columns), jnp.float32),
            pltpu.SemaphoreType.DMA((probes // GROUP,)),
        ],
        compiler_params=params,
        cost_estimate=pl.CostEstimate(
            flops=8 * probes * rows * columns, bytes_accessed=20 * probes * rows * columns, transcendentals=0
        ),
    )(*args)

    everyone = (trace + two) + (one + three)

    def again(state):
        _, turn, _, _ = state
        past = turn.astype(jnp.int32)
        diagonal = (sensor_mask + past).astype(jnp.float32) * sensor_weight + prior_mass
        made, cell = iterate_on_device(probe_signs + past, diagonal)
        return turn, turn + 1.0, made, cell

    state = (everyone[0, LANES // 2], everyone[0, LANES - 1], combined, everyone[0, 0])
    return lax.while_loop(lambda state: state[0] > 0.0, again, state)[2:]


def solution(mesh):
    return jax.shard_map(
        on_device,
        mesh=mesh,
        in_specs=(P("probe", "space", None), P("space", None), P("space", None), P("space", None)),
        out_specs=(P("probe", "space", None), P()),
        check_vma=False,
    )
```

```python
import functools

import jax
import jax.numpy as jnp
from jax import lax
from jax.experimental import pallas as pl
from jax.experimental.pallas import tpu as pltpu
from jax.sharding import PartitionSpec as P


ITERS = 4
SHIFT = 9.0
LANES = 128
GROUP = 8
CHUNKS = 2
AMPLIFIED = 600.0
VMEM_LIMIT = 16 * 1024 * 1024


VMEM = pl.BlockSpec(memory_space=pltpu.VMEM)
HBM = pl.BlockSpec(memory_space=pltpu.HBM)


def operate(vector, diagonal):
    strips = lax.axis_size("space")
    above = lax.ppermute(vector[:, -1:], "space", [(i, i + 1) for i in range(strips - 1)])
    below = lax.ppermute(vector[:, :1], "space", [(i + 1, i) for i in range(strips - 1)])
    padded = jnp.pad(jnp.concatenate([above, vector, below], axis=1), ((0, 0), (0, 0), (1, 1)))
    beside = padded[:, 2:, 1:-1] + padded[:, :-2, 1:-1]
    beside = beside + padded[:, 1:-1, 2:] + padded[:, 1:-1, :-2]
    return (4.0 + diagonal) * vector - beside


def of_everyone(values, axis):
    copies = jnp.broadcast_to(values, (lax.axis_size(axis), *values.shape))
    return jnp.sum(lax.all_to_all(copies, axis, split_axis=0, concat_axis=0, tiled=True), axis=0)


def per_probe(values):
    return of_everyone(jnp.sum(values, axis=(1, 2)), "space")


def iterate_on_device(probe_signs, diagonal):
    probes = 2.0 * probe_signs.astype(jnp.float32) - 1.0

    def iteration(_, state):
        solution, residual, direction, norm_now = state
        applied = operate(direction, diagonal)
        step = (norm_now / per_probe(direction * applied))[:, None, None]
        solution = solution + step * direction
        residual = residual - step * applied
        norm_next = per_probe(residual * residual)
        direction = residual + (norm_next / norm_now)[:, None, None] * direction
        return solution, residual, direction, norm_next

    cells = probes.shape[1] * lax.axis_size("space") * probes.shape[2]
    norm_now = jnp.full((probes.shape[0],), float(cells), jnp.float32)
    solution = lax.fori_loop(0, ITERS, iteration, (jnp.zeros_like(probes), probes, probes, norm_now))[0]
    quadratics = per_probe(probes * solution)
    trace_sum = of_everyone(jnp.sum(quadratics)[None], "probe")[0]
    return solution, trace_sum / float(probes.shape[0] * lax.axis_size("probe") * cells)


def reach(n):
    return (3, 4) if n % 2 == 0 else (4, 3)


def up_start(n, count):
    return sum(reach(m)[1] for m in range(n)) * count


def edge_of(r, n, count, refs):
    up_ref, mid_ref, *dn_refs = refs
    _, below = reach(n)
    if r < below:
        return up_ref, up_start(n, count) + r * count
    if r == below:
        return mid_ref, n * count
    return dn_refs[n], (r - below - 1) * count


def prepare_kernel(signs_hbm, mask_hbm, weight_hbm, mass_hbm, *refs):
    outs = refs[: CHUNKS + 2]
    signs_ref, mask_ref, weight_ref, mass_ref, sems = refs[CHUNKS + 2 :]
    probes, rows, columns = signs_ref.shape
    count = probes // CHUNKS
    groups = probes // GROUP
    fields = [(mask_hbm, mask_ref), (weight_hbm, weight_ref), (mass_hbm, mass_ref)]
    copies = []
    for g in range(groups):
        mine = pl.ds(g * GROUP, GROUP)
        copies.append(pltpu.make_async_copy(signs_hbm.at[mine], signs_ref.at[mine], sems.at[g]))
    for n, (src, dst) in enumerate(fields):
        copies.append(pltpu.make_async_copy(src, dst, sems.at[groups + n]))
    for copy in copies:
        copy.start()
    for g in range(groups):
        copies[g].wait()
        chunk, base = divmod(g * GROUP, count)
        for c in range(columns // LANES):
            at = slice(c * LANES, (c + 1) * LANES)
            block = 2.0 * signs_ref[g * GROUP : (g + 1) * GROUP, :, at].astype(jnp.float32) - 1.0
            block = jnp.swapaxes(block, 0, 1)
            for r in range(rows):
                ref, start = edge_of(r, chunk, count, outs)
                ref[start + base : start + base + GROUP, at] = block[r]
    for copy in copies[groups:]:
        copy.wait()
    diagonal = mask_ref[...].astype(jnp.float32) * weight_ref[...] + mass_ref[...]
    outs[0][up_start(CHUNKS, count) :, :] = diagonal
    outs[2][reach(0)[0] * count :, :] = diagonal


def powers_kernel(chunk, *refs):
    up_ref, mid_ref, below_ref, dn_ref, above_ref = refs[:5]
    if chunk:
        above_dd_ref, earlier_ref = refs[5:7]
        v1_ref, v2_ref, v3_ref, sums_ref, dd_ref, h1_ref, h2_ref, h3_ref, total_ref, part_ref = refs[7:]
    else:
        above_dd_ref = above_ref
        v1_ref, v2_ref, v3_ref, part_ref, dd_ref, h1_ref, h2_ref, h3_ref = refs[5:]
    rows, probes, columns = v1_ref.shape
    tiles = columns // LANES
    edges = [up_ref, mid_ref] + [dn_ref] * CHUNKS
    lane = lax.broadcasted_iota(jnp.int32, (GROUP, LANES), 1)
    first, last = lane == 0, lane == LANES - 1
    nothing = jnp.zeros((GROUP, LANES), jnp.float32)

    def at(c):
        return pl.ds(c * LANES, LANES)

    def spread(ref, row, to):
        line = ref[row : row + 1, :]
        dd_ref[to] = jnp.broadcast_to(line + (4.0 - SHIFT), (GROUP, columns))
        return jnp.where(jnp.broadcast_to(line[:, :LANES], (GROUP, LANES)) > 0.0, 1.0, 0.0)

    above_rows, below_rows = reach(chunk)
    low = 1 - above_rows
    for r in range(low, 0):
        in_above = spread(above_dd_ref, reach(0)[0] * probes + rows + r, r - low)
    for r in range(rows):
        spread(up_ref, up_start(CHUNKS, probes) + r, r - low)
    for r in range(rows, rows + below_rows - 1):
        in_below = spread(below_ref, up_start(CHUNKS, probes) + r - rows, r - low)
    part_ref[7 * probes :, :] = jnp.zeros((probes, LANES), jnp.float32)

    own = [None, v1_ref, v2_ref, v3_ref]
    halo = [None, h1_ref, h2_ref, h3_ref]
    spans = [(k + 1 - above_rows, rows + below_rows - 1 - k) for k in range(3)]
    place = [None]
    for begin, end in spans:
        place.append({r: n for n, r in enumerate([*range(begin, 0), *range(rows, end)])})

    def where(level, r, base):
        if level:
            if 0 <= r < rows:
                return own[level], (r, pl.ds(base, GROUP))
            return halo[level], (place[level][r], slice(None))
        if r < 0:
            return above_ref, (pl.ds((r + above_rows) * probes + base, GROUP),)
        if r >= rows:
            return below_ref, (pl.ds(up_start(chunk, probes) + (r - rows) * probes + base, GROUP),)
        ref, start = edge_of(r, chunk, probes, edges)
        return ref, (pl.ds(start + base, GROUP),)

    def sideways(v):
        left = [pltpu.roll(t, 1, 1) for t in v]
        right = [pltpu.roll(t, LANES - 1, 1) for t in v]
        out = []
        for c in range(tiles):
            a = jnp.where(first, left[c - 1] if c else nothing, left[c])
            b = jnp.where(last, right[c + 1] if c + 1 < tiles else nothing, right[c])
            out.append(a + b)
        return out

    def group(g, carry):
        base = pl.multiple_of(g * GROUP, GROUP)

        def line(level, r):
            ref, index = where(level, r, base)
            return [ref[index + (at(c),)] for c in range(tiles)]

        totals = []
        for level, (begin, end) in enumerate(spans):
            cross, square = nothing, nothing
            before, here = line(level, begin - 1), line(level, begin)
            for r in range(begin, end):
                after = line(level, r + 1)
                side = sideways(here)
                ref, index = where(level + 1, r, base)
                for c in range(tiles):
                    value = dd_ref[r - low, :, at(c)] * here[c] - (side[c] + (before[c] + after[c]))
                    if r < 0:
                        value = in_above * value
                    if r >= rows:
                        value = in_below * value
                    ref[index + (at(c),)] = value
                    if 0 <= r < rows:
                        cross = cross + here[c] * value
                        square = square + value * value
                before, here = here, after
            totals += [cross, square]
        quad = nothing
        if below_rows < above_rows:
            beyond = line(3, -1)
        for r in range(rows):
            here = line(3, r)
            if below_rows > above_rows:
                beyond = line(3, r + 1)
            right = [pltpu.roll(t, LANES - 1, 1) for t in here]
            for c in range(tiles):
                beside = jnp.where(last, right[c + 1] if c + 1 < tiles else nothing, right[c]) + beyond[c]
                quad = quad + here[c] * (dd_ref[r - low, :, at(c)] * here[c] - (beside + beside))
            beyond = here
        totals.append(quad)
        for k, total in enumerate(totals):
            part_ref[pl.ds(k * probes + base, GROUP), :] = total
        return carry

    lax.fori_loop(0, probes // GROUP, group, 0)
    if not chunk:
        return
    for k in range(8):
        begin = k * CHUNKS * probes
        total_ref[begin : begin + probes, :] = earlier_ref[k * probes : (k + 1) * probes, :]
        total_ref[begin + probes : begin + 2 * probes, :] = part_ref[k * probes : (k + 1) * probes, :]
    ones = jnp.ones((GROUP, LANES), jnp.float32)
    line = lax.dot_general(
        ones, total_ref[...], (((1,), (1,)), ((), ())),
        precision=lax.Precision.HIGHEST, preferred_element_type=jnp.float32,
    )
    sums_ref[...] = jnp.broadcast_to(line[None, 0:1, :], sums_ref.shape)


def quadratic(c, moments):
    total = None
    n = len(c)
    for s in range(2 * n - 1):
        pairs = [c[a] * c[s - a] for a in range(max(0, s - n + 1), min(n, s + 1))]
        term = functools.reduce(lambda a, b: a + b, pairs) * moments[s]
        total = term if total is None else total + term
    return total


def coefficients(mu, shift):
    zero = jnp.zeros_like(mu[0])
    size = [jnp.abs(m) for m in mu]
    moved = [mu[k + 1] + shift * mu[k] for k in range(2 * ITERS - 1)]
    moved_size = [size[k + 1] + shift * size[k] for k in range(2 * ITERS - 1)]
    residual = [jnp.ones_like(mu[0])]
    direction = residual
    solution = [zero] * ITERS
    norm_now = mu[0]
    lost = jnp.ones_like(mu[0])
    amplified = zero
    for i in range(ITERS):
        curvature = quadratic(direction, moved)
        step = norm_now / curvature
        loss = quadratic([jnp.abs(d) for d in direction], moved_size) / jnp.abs(curvature)
        length = jnp.sqrt(jnp.abs(quadratic(direction, mu)))
        amplified = amplified + (loss + lost) * (jnp.abs(step) * length)
        solution = [x + step * direction[k] if k <= i else x for k, x in enumerate(solution)]
        if i + 1 < ITERS:
            applied = [shift * d for d in direction] + [zero]
            applied = [a + (direction[k - 1] if k else zero) for k, a in enumerate(applied)]
            residual = [r - step * a for r, a in zip(residual + [zero], applied)]
            norm_next = quadratic(residual, mu)
            lost = quadratic([jnp.abs(r) for r in residual], size) / jnp.abs(norm_next)
            ratio = norm_next / norm_now
            direction = [r + ratio * d for r, d in zip(residual, direction + [zero])]
            norm_now = norm_next
    for k in range(ITERS):
        amplified = amplified + jnp.abs(solution[k]) * jnp.sqrt(size[2 * k])
    length = jnp.sqrt(quadratic(solution, mu))
    return solution, amplified / length


def solve_kernel(cells, groups, sums_ref, coef_ref, trace_ref):
    row = jnp.sum(sums_ref[...], axis=0)
    width = row.shape[1]
    probes = width // 8
    row = jnp.broadcast_to(row, (8, width))
    mu = [jnp.full((8, LANES), cells, jnp.float32)]
    for k in range(2 * ITERS - 1):
        moved = pltpu.roll(row, width - k * probes, 1) if k else row
        mu.append(moved[:, :LANES])
    coef, amplified = coefficients(mu, SHIFT)
    sub = lax.broadcasted_iota(jnp.int32, (8, LANES), 0)
    lane = lax.broadcasted_iota(jnp.int32, (8, LANES), 1)
    packed = jnp.zeros((8, LANES), jnp.float32)
    trace = jnp.zeros((8, LANES), jnp.float32)
    for k in range(ITERS):
        packed = jnp.where(sub == k, coef[k], packed)
        trace = trace + coef[k] * mu[k]
    trace = jnp.where(lane < probes, trace, 0.0)
    total = jnp.sum(trace, axis=1, keepdims=True) / (float(probes * groups) * cells)
    unsafe = jnp.where(amplified < AMPLIFIED, 0.0, 1.0)
    unsafe = jnp.max(jnp.where(lane < probes, unsafe, 0.0), axis=1, keepdims=True)
    both = jnp.where(lane < LANES // 2, jnp.broadcast_to(total, lane.shape), jnp.broadcast_to(unsafe, lane.shape))
    trace_ref[...] = jnp.where(lane < LANES - 1, both, 0.0)[0:1]
    across = jnp.transpose(packed)
    for k in range(ITERS):
        coef_ref[k * probes : (k + 1) * probes, :] = jnp.broadcast_to(across[:probes, k : k + 1], (probes, LANES))


def combine_kernel(coef_ref, *refs):
    edges = refs[: CHUNKS + 2]
    powers = [refs[CHUNKS + 2 + 3 * n : CHUNKS + 5 + 3 * n] for n in range(CHUNKS)]
    out_ref, made_ref, sems = refs[4 * CHUNKS + 2 :]
    probes, rows, columns = made_ref.shape
    count = probes // CHUNKS

    def copy(g):
        mine = pl.ds(g * GROUP, GROUP)
        return pltpu.make_async_copy(made_ref.at[mine], out_ref.at[mine], sems.at[g])

    for g in range(probes // GROUP):
        base = g * GROUP
        chunk, local = divmod(base, count)
        v1_ref, v2_ref, v3_ref = powers[chunk]
        mine = slice(local, local + GROUP)
        c = [coef_ref[k * probes + base : k * probes + base + GROUP, :] for k in range(ITERS)]
        for t in range(columns // LANES):
            at = slice(t * LANES, (t + 1) * LANES)
            made = []
            for r in range(rows):
                ref, start = edge_of(r, chunk, count, edges)
                probe = ref[start + local : start + local + GROUP, at]
                made.append(
                    (c[0] * probe + c[1] * v1_ref[r, mine, at]) + (c[2] * v2_ref[r, mine, at] + c[3] * v3_ref[r, mine, at])
                )
            made_ref[base : base + GROUP, :, at] = jnp.swapaxes(jnp.stack(made), 0, 1)
        copy(g).start()
    for g in range(probes // GROUP):
        copy(g).wait()


def on_device(probe_signs, sensor_mask, sensor_weight, prior_mass):
    probes, rows, columns = probe_signs.shape
    strips = lax.axis_size("space")
    groups = lax.axis_size("probe")
    count = probes // CHUNKS
    params = pltpu.CompilerParams(vmem_limit_bytes=VMEM_LIMIT)

    def shaped(*shape):
        return jax.ShapeDtypeStruct(shape, jnp.float32)

    edges = pl.pallas_call(
        prepare_kernel,
        in_specs=[HBM] * 4,
        out_specs=[VMEM] * (CHUNKS + 2),
        out_shape=[shaped(up_start(CHUNKS, count) + rows, columns), shaped(probes, columns)]
        + [shaped(reach(n)[0] * count + (0 if n else rows), columns) for n in range(CHUNKS)],
        scratch_shapes=[
            pltpu.VMEM((probes, rows, columns), jnp.int32),
            pltpu.VMEM((rows, columns), jnp.int32),
            pltpu.VMEM((rows, columns), jnp.float32),
            pltpu.VMEM((rows, columns), jnp.float32),
            pltpu.SemaphoreType.DMA((probes // GROUP + 3,)),
        ],
        compiler_params=params,
    )(probe_signs, sensor_mask, sensor_weight, prior_mass)
    up, mid, *downs = edges
    below = lax.ppermute(up, "space", [(i + 1, i) for i in range(strips - 1)])
    above = []
    for dn in downs:
        above.append(lax.ppermute(dn, "space", [(i, i + 1) for i in range(strips - 1)]))

    field = shaped(rows, count, columns)
    powers = []
    for n in range(CHUNKS):
        args = [up, mid, below, downs[n], above[n]]
        sums = shaped(8 * count, LANES)
        scratch = [pltpu.VMEM((size, GROUP, columns), jnp.float32) for size in (rows + 5, 5, 3, 1)]
        if n:
            args += [above[0], powers[0][3]]
            sums = shaped(strips, 1, 8 * probes)
            scratch += [pltpu.VMEM((8 * probes, LANES), jnp.float32), pltpu.VMEM((8 * count, LANES), jnp.float32)]
        powers.append(
            pl.pallas_call(
                functools.partial(powers_kernel, n),
                in_specs=[VMEM] * len(args),
                out_specs=[VMEM] * 4,
                out_shape=[field, field, field, sums],
                scratch_shapes=scratch,
                compiler_params=params,
            )(*args)
        )

    sums = lax.all_to_all(powers[-1][3], "space", split_axis=0, concat_axis=0, tiled=True)

    cells = float(rows * strips * columns)
    coef, trace = pl.pallas_call(
        functools.partial(solve_kernel, cells, groups),
        in_specs=[VMEM],
        out_specs=[VMEM, VMEM],
        out_shape=[shaped(ITERS * probes, LANES), shaped(1, LANES)],
        compiler_params=params,
    )(sums)

    one, two, three = [
        lax.ppermute(trace, "probe", [(i, (i + k) % groups) for i in range(groups)])
        for k in range(1, groups)
    ]

    args = [coef, *edges]
    for power in powers:
        args += power[:3]
    combined = pl.pallas_call(
        combine_kernel,
        in_specs=[VMEM] * len(args),
        out_specs=HBM,
        out_shape=shaped(probes, rows, columns),
        scratch_shapes=[
            pltpu.VMEM((probes, rows, columns), jnp.float32),
            pltpu.SemaphoreType.DMA((probes // GROUP,)),
        ],
        compiler_params=params,
        cost_estimate=pl.CostEstimate(
            flops=8 * probes * rows * columns, bytes_accessed=20 * probes * rows * columns, transcendentals=0
        ),
    )(*args)

    everyone = (trace + two) + (one + three)

    def again(state):
        _, turn, _, _ = state
        past = turn.astype(jnp.int32)
        diagonal = (sensor_mask + past).astype(jnp.float32) * sensor_weight + prior_mass
        made, cell = iterate_on_device(probe_signs + past, diagonal)
        return turn, turn + 1.0, made, cell

    state = (everyone[0, LANES // 2], everyone[0, LANES - 1], combined, everyone[0, 0])
    return lax.while_loop(lambda state: state[0] > 0.0, again, state)[2:]


def solution(mesh):
    return jax.shard_map(
        on_device,
        mesh=mesh,
        in_specs=(P("probe", "space", None), P("space", None), P("space", None), P("space", None)),
        out_specs=(P("probe", "space", None), P()),
        check_vma=False,
    )
```

```python
import functools

import jax
import jax.numpy as jnp
from jax import lax
from jax.experimental import pallas as pl
from jax.experimental.pallas import tpu as pltpu
from jax.sharding import PartitionSpec as P


ITERS = 4
SHIFT = 9.0
LANES = 128
GROUP = 8
CHUNKS = 2
ROWS = 8
AMPLIFIED = 600.0
VMEM_LIMIT = 16 * 1024 * 1024


VMEM = pl.BlockSpec(memory_space=pltpu.VMEM)
HBM = pl.BlockSpec(memory_space=pltpu.HBM)


def operate(vector, diagonal):
    strips = lax.axis_size("space")
    above = lax.ppermute(vector[:, -1:], "space", [(i, i + 1) for i in range(strips - 1)])
    below = lax.ppermute(vector[:, :1], "space", [(i + 1, i) for i in range(strips - 1)])
    padded = jnp.pad(jnp.concatenate([above, vector, below], axis=1), ((0, 0), (0, 0), (1, 1)))
    beside = padded[:, 2:, 1:-1] + padded[:, :-2, 1:-1]
    beside = beside + padded[:, 1:-1, 2:] + padded[:, 1:-1, :-2]
    return (4.0 + diagonal) * vector - beside


def of_everyone(values, axis):
    copies = jnp.broadcast_to(values, (lax.axis_size(axis), *values.shape))
    return jnp.sum(lax.all_to_all(copies, axis, split_axis=0, concat_axis=0, tiled=True), axis=0)


def per_probe(values):
    return of_everyone(jnp.sum(values, axis=(1, 2)), "space")


def iterate_on_device(probe_signs, diagonal):
    probes = 2.0 * probe_signs.astype(jnp.float32) - 1.0

    def iteration(_, state):
        solution, residual, direction, norm_now = state
        applied = operate(direction, diagonal)
        step = (norm_now / per_probe(direction * applied))[:, None, None]
        solution = solution + step * direction
        residual = residual - step * applied
        norm_next = per_probe(residual * residual)
        direction = residual + (norm_next / norm_now)[:, None, None] * direction
        return solution, residual, direction, norm_next

    cells = probes.shape[1] * lax.axis_size("space") * probes.shape[2]
    norm_now = jnp.full((probes.shape[0],), float(cells), jnp.float32)
    solution = lax.fori_loop(0, ITERS, iteration, (jnp.zeros_like(probes), probes, probes, norm_now))[0]
    quadratics = per_probe(probes * solution)
    trace_sum = of_everyone(jnp.sum(quadratics)[None], "probe")[0]
    return solution, trace_sum / float(probes.shape[0] * lax.axis_size("probe") * cells)


def reach(n):
    return (3, 4) if n % 2 == 0 else (4, 3)


def up_start(n, count):
    return sum(reach(m)[1] for m in range(n)) * count


def edge_of(r, n, count, refs):
    up_ref, mid_ref, *dn_refs = refs
    _, below = reach(n)
    if r < below:
        return up_ref, up_start(n, count) + r * count
    if r == below:
        return mid_ref, n * count
    return dn_refs[n], (r - below - 1) * count


def prepare_kernel(signs_hbm, mask_hbm, weight_hbm, mass_hbm, *refs):
    outs = refs[: CHUNKS + 2]
    signs_ref, mask_ref, weight_ref, mass_ref, sems = refs[CHUNKS + 2 :]
    probes, rows, columns = signs_ref.shape
    count = probes // CHUNKS
    groups = probes // GROUP
    fields = [(mask_hbm, mask_ref), (weight_hbm, weight_ref), (mass_hbm, mass_ref)]
    copies = []
    for g in range(groups):
        mine = pl.ds(g * GROUP, GROUP)
        copies.append(pltpu.make_async_copy(signs_hbm.at[mine], signs_ref.at[mine], sems.at[g]))
    for n, (src, dst) in enumerate(fields):
        copies.append(pltpu.make_async_copy(src, dst, sems.at[groups + n]))
    for copy in copies:
        copy.start()
    for g in range(groups):
        copies[g].wait()
        chunk, base = divmod(g * GROUP, count)
        for c in range(columns // LANES):
            at = slice(c * LANES, (c + 1) * LANES)
            block = 2.0 * signs_ref[g * GROUP : (g + 1) * GROUP, :, at].astype(jnp.float32) - 1.0
            block = jnp.swapaxes(block, 0, 1)
            for r in range(rows):
                ref, start = edge_of(r, chunk, count, outs)
                ref[start + base : start + base + GROUP, at] = block[r]
    for copy in copies[groups:]:
        copy.wait()
    diagonal = mask_ref[...].astype(jnp.float32) * weight_ref[...] + mass_ref[...]
    outs[0][up_start(CHUNKS, count) :, :] = diagonal
    outs[2][reach(0)[0] * count :, :] = diagonal


def owner(level, r, rows):
    return 0 if level <= r < rows - level else 1 if r >= rows - level else 2


def kept(stage, level, rows):
    return [(level, rows - 2 * level), (rows - level, level), (0, level)][stage]


def powers_kernel(stage, chunk, final, *refs):
    refs = list(refs)
    edges = [refs.pop(0), refs.pop(0)]
    dn_ref = refs.pop(0)
    edges += [dn_ref] * CHUNKS
    up_ref = edges[0]
    side_ref = refs.pop(0) if stage else None
    far_ref = refs.pop(0) if stage else None
    middle = [None] + [refs.pop(0) for _ in range(ITERS - 1)] if stage else None
    before_ref = refs.pop(0) if stage else None
    earlier_ref = refs.pop(0) if final else None
    own = [None] + [refs.pop(0) for _ in range(ITERS - 1)]
    if final:
        sums_ref, dd_ref, h1_ref, h2_ref, h3_ref, total_ref, part_ref = refs
    else:
        part_ref, dd_ref, h1_ref, h2_ref, h3_ref = refs
    halo = [None, h1_ref, h2_ref, h3_ref]
    _, probes, columns = own[1].shape
    rows = ROWS
    tiles = columns // LANES
    lane = lax.broadcasted_iota(jnp.int32, (GROUP, LANES), 1)
    first, last = lane == 0, lane == LANES - 1
    nothing = jnp.zeros((GROUP, LANES), jnp.float32)
    above_rows, below_rows = reach(chunk)

    def at(c):
        return pl.ds(c * LANES, LANES)

    spans = []
    for level in range(1, ITERS):
        begin, end = level - above_rows, rows + below_rows - level
        spans.append([r for r in range(begin, end) if owner(level, r, rows) == stage])
    upward = below_rows > above_rows
    corner = [3] if upward else [4]
    quads = [corner, range(corner[0] + 1, rows), range(corner[0])][stage]
    low = min(min(spans[0]), min(quads))
    high = max(max(spans[0]), max(quads))

    inside = None
    for r in range(low, high + 1):
        if r < 0:
            ref, row = far_ref, reach(0)[0] * probes + rows + r
        elif r < rows:
            ref, row = up_ref, up_start(CHUNKS, probes) + r
        else:
            ref, row = far_ref, up_start(CHUNKS, probes) + r - rows
        line = ref[row : row + 1, :]
        dd_ref[r - low] = jnp.broadcast_to(line + (4.0 - SHIFT), (GROUP, columns))
        if not 0 <= r < rows:
            inside = jnp.where(jnp.broadcast_to(line[:, :LANES], (GROUP, LANES)) > 0.0, 1.0, 0.0)

    def where(level, r, base):
        mine = pl.ds(base, GROUP)
        if level:
            if not 0 <= r < rows:
                n = r - rows if r >= rows else r + above_rows - level
                return halo[level], (n, slice(None))
            by = owner(level, r, rows)
            source = own if by == stage else middle
            return source[level], (r - kept(by, level, rows)[0], mine)
        if r < 0:
            return side_ref, (pl.ds((r + above_rows) * probes + base, GROUP),)
        if r >= rows:
            return side_ref, (pl.ds(up_start(chunk, probes) + (r - rows) * probes + base, GROUP),)
        ref, start = edge_of(r, chunk, probes, edges)
        return ref, (pl.ds(start + base, GROUP),)

    def sideways(v):
        left = [pltpu.roll(t, 1, 1) for t in v]
        right = [pltpu.roll(t, LANES - 1, 1) for t in v]
        out = []
        for c in range(tiles):
            a = jnp.where(first, left[c - 1] if c else nothing, left[c])
            b = jnp.where(last, right[c + 1] if c + 1 < tiles else nothing, right[c])
            out.append(a + b)
        return out

    def group(g, carry):
        base = pl.multiple_of(g * GROUP, GROUP)

        def line(level, r):
            ref, index = where(level, r, base)
            return [ref[index + (at(c),)] for c in range(tiles)]

        totals = []
        for level, span in enumerate(spans):
            cross, square = nothing, nothing
            before, here = line(level, span[0] - 1), line(level, span[0])
            for r in span:
                after = line(level, r + 1)
                side = sideways(here)
                ref, index = where(level + 1, r, base)
                for c in range(tiles):
                    value = dd_ref[r - low, :, at(c)] * here[c] - (side[c] + (before[c] + after[c]))
                    if not 0 <= r < rows:
                        value = inside * value
                    ref[index + (at(c),)] = value
                    if 0 <= r < rows:
                        cross = cross + here[c] * value
                        square = square + value * value
                before, here = here, after
            totals += [cross, square]
        quad = nothing
        for r in quads:
            here = line(3, r)
            beyond = line(3, r + 1 if upward else r - 1)
            right = [pltpu.roll(t, LANES - 1, 1) for t in here]
            for c in range(tiles):
                beside = jnp.where(last, right[c + 1] if c + 1 < tiles else nothing, right[c]) + beyond[c]
                quad = quad + here[c] * (dd_ref[r - low, :, at(c)] * here[c] - (beside + beside))
        totals.append(quad)
        for k, total in enumerate(totals):
            mine = pl.ds(k * probes + base, GROUP)
            part_ref[mine, :] = total + before_ref[mine, :] if stage else total
        return carry

    lax.fori_loop(0, probes // GROUP, group, 0)
    part_ref[7 * probes :, :] = jnp.zeros((probes, LANES), jnp.float32)
    if not final:
        return
    for k in range(8):
        begin = k * CHUNKS * probes
        total_ref[begin : begin + probes, :] = earlier_ref[k * probes : (k + 1) * probes, :]
        total_ref[begin + probes : begin + 2 * probes, :] = part_ref[k * probes : (k + 1) * probes, :]
    ones = jnp.ones((GROUP, LANES), jnp.float32)
    line = lax.dot_general(
        ones, total_ref[...], (((1,), (1,)), ((), ())),
        precision=lax.Precision.HIGHEST, preferred_element_type=jnp.float32,
    )
    sums_ref[...] = jnp.broadcast_to(line[None, 0:1, :], sums_ref.shape)


def quadratic(c, moments):
    total = None
    n = len(c)
    for s in range(2 * n - 1):
        pairs = [c[a] * c[s - a] for a in range(max(0, s - n + 1), min(n, s + 1))]
        term = functools.reduce(lambda a, b: a + b, pairs) * moments[s]
        total = term if total is None else total + term
    return total


def coefficients(mu, shift):
    zero = jnp.zeros_like(mu[0])
    size = [jnp.abs(m) for m in mu]
    moved = [mu[k + 1] + shift * mu[k] for k in range(2 * ITERS - 1)]
    moved_size = [size[k + 1] + shift * size[k] for k in range(2 * ITERS - 1)]
    residual = [jnp.ones_like(mu[0])]
    direction = residual
    solution = [zero] * ITERS
    norm_now = mu[0]
    lost = jnp.ones_like(mu[0])
    amplified = zero
    for i in range(ITERS):
        curvature = quadratic(direction, moved)
        step = norm_now / curvature
        loss = quadratic([jnp.abs(d) for d in direction], moved_size) / jnp.abs(curvature)
        length = jnp.sqrt(jnp.abs(quadratic(direction, mu)))
        amplified = amplified + (loss + lost) * (jnp.abs(step) * length)
        solution = [x + step * direction[k] if k <= i else x for k, x in enumerate(solution)]
        if i + 1 < ITERS:
            applied = [shift * d for d in direction] + [zero]
            applied = [a + (direction[k - 1] if k else zero) for k, a in enumerate(applied)]
            residual = [r - step * a for r, a in zip(residual + [zero], applied)]
            norm_next = quadratic(residual, mu)
            lost = quadratic([jnp.abs(r) for r in residual], size) / jnp.abs(norm_next)
            ratio = norm_next / norm_now
            direction = [r + ratio * d for r, d in zip(residual, direction + [zero])]
            norm_now = norm_next
    for k in range(ITERS):
        amplified = amplified + jnp.abs(solution[k]) * jnp.sqrt(size[2 * k])
    length = jnp.sqrt(quadratic(solution, mu))
    return solution, amplified / length


def solve_kernel(cells, groups, sums_ref, coef_ref, trace_ref):
    row = jnp.sum(sums_ref[...], axis=0)
    width = row.shape[1]
    probes = width // 8
    row = jnp.broadcast_to(row, (8, width))
    mu = [jnp.full((8, LANES), cells, jnp.float32)]
    for k in range(2 * ITERS - 1):
        moved = pltpu.roll(row, width - k * probes, 1) if k else row
        mu.append(moved[:, :LANES])
    coef, amplified = coefficients(mu, SHIFT)
    sub = lax.broadcasted_iota(jnp.int32, (8, LANES), 0)
    lane = lax.broadcasted_iota(jnp.int32, (8, LANES), 1)
    packed = jnp.zeros((8, LANES), jnp.float32)
    trace = jnp.zeros((8, LANES), jnp.float32)
    for k in range(ITERS):
        packed = jnp.where(sub == k, coef[k], packed)
        trace = trace + coef[k] * mu[k]
    trace = jnp.where(lane < probes, trace, 0.0)
    total = jnp.sum(trace, axis=1, keepdims=True) / (float(probes * groups) * cells)
    unsafe = jnp.where(amplified < AMPLIFIED, 0.0, 1.0)
    unsafe = jnp.max(jnp.where(lane < probes, unsafe, 0.0), axis=1, keepdims=True)
    both = jnp.where(lane < LANES // 2, jnp.broadcast_to(total, lane.shape), jnp.broadcast_to(unsafe, lane.shape))
    trace_ref[...] = jnp.where(lane < LANES - 1, both, 0.0)[0:1]
    across = jnp.transpose(packed)
    for k in range(ITERS):
        coef_ref[k * probes : (k + 1) * probes, :] = jnp.broadcast_to(across[:probes, k : k + 1], (probes, LANES))


def combine_kernel(coef_ref, *refs):
    edges = refs[: CHUNKS + 2]
    powers = [refs[CHUNKS + 2 + 9 * n : CHUNKS + 11 + 9 * n] for n in range(CHUNKS)]
    out_ref, made_ref, sems = refs[10 * CHUNKS + 2 :]
    probes, rows, columns = made_ref.shape
    count = probes // CHUNKS

    def copy(g):
        mine = pl.ds(g * GROUP, GROUP)
        return pltpu.make_async_copy(made_ref.at[mine], out_ref.at[mine], sems.at[g])

    for g in range(probes // GROUP):
        base = g * GROUP
        chunk, local = divmod(base, count)

        def power(level, r):
            by = owner(level, r, rows)
            return powers[chunk][3 * by + level - 1][r - kept(by, level, rows)[0], mine, at]

        mine = slice(local, local + GROUP)
        c = [coef_ref[k * probes + base : k * probes + base + GROUP, :] for k in range(ITERS)]
        for t in range(columns // LANES):
            at = slice(t * LANES, (t + 1) * LANES)
            made = []
            for r in range(rows):
                ref, start = edge_of(r, chunk, count, edges)
                probe = ref[start + local : start + local + GROUP, at]
                made.append(
                    (c[0] * probe + c[1] * power(1, r)) + (c[2] * power(2, r) + c[3] * power(3, r))
                )
            made_ref[base : base + GROUP, :, at] = jnp.swapaxes(jnp.stack(made), 0, 1)
        copy(g).start()
    for g in range(probes // GROUP):
        copy(g).wait()


def on_device(probe_signs, sensor_mask, sensor_weight, prior_mass):
    probes, rows, columns = probe_signs.shape
    strips = lax.axis_size("space")
    groups = lax.axis_size("probe")
    count = probes // CHUNKS
    params = pltpu.CompilerParams(vmem_limit_bytes=VMEM_LIMIT)

    def shaped(*shape):
        return jax.ShapeDtypeStruct(shape, jnp.float32)

    edges = pl.pallas_call(
        prepare_kernel,
        in_specs=[HBM] * 4,
        out_specs=[VMEM] * (CHUNKS + 2),
        out_shape=[shaped(up_start(CHUNKS, count) + rows, columns), shaped(probes, columns)]
        + [shaped(reach(n)[0] * count + (0 if n else rows), columns) for n in range(CHUNKS)],
        scratch_shapes=[
            pltpu.VMEM((probes, rows, columns), jnp.int32),
            pltpu.VMEM((rows, columns), jnp.int32),
            pltpu.VMEM((rows, columns), jnp.float32),
            pltpu.VMEM((rows, columns), jnp.float32),
            pltpu.SemaphoreType.DMA((probes // GROUP + 3,)),
        ],
        compiler_params=params,
    )(probe_signs, sensor_mask, sensor_weight, prior_mass)
    up, mid, *downs = edges
    below = lax.ppermute(up, "space", [(i + 1, i) for i in range(strips - 1)])
    above = []
    for dn in downs:
        above.append(lax.ppermute(dn, "space", [(i, i + 1) for i in range(strips - 1)]))

    made = [[], []]
    parts = [None, None]
    for stage in range(3):
        for n in range(CHUNKS):
            final = stage == 2 and n == CHUNKS - 1
            args = [up, mid, downs[n]]
            if stage:
                args += [below, below] if stage == 1 else [above[n], above[0]]
                args += [*made[n][:3], parts[n]]
            if final:
                args.append(parts[0])
            outs = [shaped(kept(stage, level, rows)[1], count, columns) for level in range(1, ITERS)]
            outs.append(shaped(strips, 1, 8 * probes) if final else shaped(8 * count, LANES))
            scratch = [pltpu.VMEM((size, GROUP, columns), jnp.float32) for size in (rows + 5, 3, 2, 1)]
            if final:
                scratch += [pltpu.VMEM((8 * probes, LANES), jnp.float32), pltpu.VMEM((8 * count, LANES), jnp.float32)]
            *fresh, parts[n] = pl.pallas_call(
                functools.partial(powers_kernel, stage, n, final),
                in_specs=[VMEM] * len(args),
                out_specs=[VMEM] * len(outs),
                out_shape=outs,
                scratch_shapes=scratch,
                compiler_params=params,
            )(*args)
            made[n] += fresh

    sums = lax.all_to_all(parts[-1], "space", split_axis=0, concat_axis=0, tiled=True)

    cells = float(rows * strips * columns)
    coef, trace = pl.pallas_call(
        functools.partial(solve_kernel, cells, groups),
        in_specs=[VMEM],
        out_specs=[VMEM, VMEM],
        out_shape=[shaped(ITERS * probes, LANES), shaped(1, LANES)],
        compiler_params=params,
    )(sums)

    one, two, three = [
        lax.ppermute(trace, "probe", [(i, (i + k) % groups) for i in range(groups)])
        for k in range(1, groups)
    ]

    args = [coef, *edges]
    for fresh in made:
        args += fresh
    combined = pl.pallas_call(
        combine_kernel,
        in_specs=[VMEM] * len(args),
        out_specs=HBM,
        out_shape=shaped(probes, rows, columns),
        scratch_shapes=[
            pltpu.VMEM((probes, rows, columns), jnp.float32),
            pltpu.SemaphoreType.DMA((probes // GROUP,)),
        ],
        compiler_params=params,
        cost_estimate=pl.CostEstimate(
            flops=8 * probes * rows * columns, bytes_accessed=20 * probes * rows * columns, transcendentals=0
        ),
    )(*args)

    everyone = (trace + two) + (one + three)

    def again(state):
        _, turn, _, _ = state
        past = turn.astype(jnp.int32)
        diagonal = (sensor_mask + past).astype(jnp.float32) * sensor_weight + prior_mass
        made, cell = iterate_on_device(probe_signs + past, diagonal)
        return turn, turn + 1.0, made, cell

    state = (everyone[0, LANES // 2], everyone[0, LANES - 1], combined, everyone[0, 0])
    return lax.while_loop(lambda state: state[0] > 0.0, again, state)[2:]


def solution(mesh):
    return jax.shard_map(
        on_device,
        mesh=mesh,
        in_specs=(P("probe", "space", None), P("space", None), P("space", None), P("space", None)),
        out_specs=(P("probe", "space", None), P()),
        check_vma=False,
    )
```

```python
import functools

import jax
import jax.numpy as jnp
from jax import lax
from jax.experimental import pallas as pl
from jax.experimental.pallas import tpu as pltpu
from jax.sharding import PartitionSpec as P


ITERS = 4
SHIFT = 9.0
LANES = 128
GROUP = 8
CHUNKS = 2
ROWS = 8
AMPLIFIED = 600.0
VMEM_LIMIT = 16 * 1024 * 1024


VMEM = pl.BlockSpec(memory_space=pltpu.VMEM)
HBM = pl.BlockSpec(memory_space=pltpu.HBM)


def operate(vector, diagonal):
    strips = lax.axis_size("space")
    above = lax.ppermute(vector[:, -1:], "space", [(i, i + 1) for i in range(strips - 1)])
    below = lax.ppermute(vector[:, :1], "space", [(i + 1, i) for i in range(strips - 1)])
    padded = jnp.pad(jnp.concatenate([above, vector, below], axis=1), ((0, 0), (0, 0), (1, 1)))
    beside = padded[:, 2:, 1:-1] + padded[:, :-2, 1:-1]
    beside = beside + padded[:, 1:-1, 2:] + padded[:, 1:-1, :-2]
    return (4.0 + diagonal) * vector - beside


def of_everyone(values, axis):
    copies = jnp.broadcast_to(values, (lax.axis_size(axis), *values.shape))
    return jnp.sum(lax.all_to_all(copies, axis, split_axis=0, concat_axis=0, tiled=True), axis=0)


def per_probe(values):
    return of_everyone(jnp.sum(values, axis=(1, 2)), "space")


def iterate_on_device(probe_signs, diagonal):
    probes = 2.0 * probe_signs.astype(jnp.float32) - 1.0

    def iteration(_, state):
        solution, residual, direction, norm_now = state
        applied = operate(direction, diagonal)
        step = (norm_now / per_probe(direction * applied))[:, None, None]
        solution = solution + step * direction
        residual = residual - step * applied
        norm_next = per_probe(residual * residual)
        direction = residual + (norm_next / norm_now)[:, None, None] * direction
        return solution, residual, direction, norm_next

    cells = probes.shape[1] * lax.axis_size("space") * probes.shape[2]
    norm_now = jnp.full((probes.shape[0],), float(cells), jnp.float32)
    solution = lax.fori_loop(0, ITERS, iteration, (jnp.zeros_like(probes), probes, probes, norm_now))[0]
    quadratics = per_probe(probes * solution)
    trace_sum = of_everyone(jnp.sum(quadratics)[None], "probe")[0]
    return solution, trace_sum / float(probes.shape[0] * lax.axis_size("probe") * cells)


def reach(n):
    return (4, 3) if n % 2 == 0 else (3, 4)


def up_start(n, count):
    return sum(reach(m)[1] for m in range(n)) * count


def edge_of(r, n, count, refs):
    up_ref, mid_ref, *dn_refs = refs
    _, below = reach(n)
    if r < below:
        return up_ref, up_start(n, count) + r * count
    if r == below:
        return mid_ref, n * count
    return dn_refs[n], (r - below - 1) * count


def prepare_kernel(signs_hbm, mask_hbm, weight_hbm, mass_hbm, *refs):
    outs = refs[: CHUNKS + 2]
    signs_ref, mask_ref, weight_ref, mass_ref, sems = refs[CHUNKS + 2 :]
    probes, rows, columns = signs_ref.shape
    count = probes // CHUNKS
    groups = probes // GROUP
    fields = [(mask_hbm, mask_ref), (weight_hbm, weight_ref), (mass_hbm, mass_ref)]
    copies = []
    for g in range(groups):
        mine = pl.ds(g * GROUP, GROUP)
        copies.append(pltpu.make_async_copy(signs_hbm.at[mine], signs_ref.at[mine], sems.at[g]))
    for n, (src, dst) in enumerate(fields):
        copies.append(pltpu.make_async_copy(src, dst, sems.at[groups + n]))
    for copy in copies:
        copy.start()
    for g in range(groups):
        copies[g].wait()
        chunk, base = divmod(g * GROUP, count)
        for c in range(columns // LANES):
            at = slice(c * LANES, (c + 1) * LANES)
            block = 2.0 * signs_ref[g * GROUP : (g + 1) * GROUP, :, at].astype(jnp.float32) - 1.0
            block = jnp.swapaxes(block, 0, 1)
            for r in range(rows):
                ref, start = edge_of(r, chunk, count, outs)
                ref[start + base : start + base + GROUP, at] = block[r]
    for copy in copies[groups:]:
        copy.wait()
    diagonal = mask_ref[...].astype(jnp.float32) * weight_ref[...] + mass_ref[...]
    outs[0][up_start(CHUNKS, count) :, :] = diagonal
    outs[2][reach(0)[0] * count :, :] = diagonal


def owner(level, r, rows):
    return 0 if level <= r < rows - level else 1 if r >= rows - level else 2


def kept(stage, level, rows):
    return [(level, rows - 2 * level), (rows - level, level), (0, level)][stage]


def powers_kernel(stage, chunk, final, *refs):
    refs = list(refs)
    edges = [refs.pop(0), refs.pop(0)]
    dn_ref = refs.pop(0)
    edges += [dn_ref] * CHUNKS
    up_ref = edges[0]
    side_ref = refs.pop(0) if stage else None
    far_ref = refs.pop(0) if stage else None
    middle = [None] + [refs.pop(0) for _ in range(ITERS - 1)] if stage else None
    before_ref = refs.pop(0) if stage else None
    earlier_ref = refs.pop(0) if final else None
    own = [None] + [refs.pop(0) for _ in range(ITERS - 1)]
    if final:
        sums_ref, dd_ref, h1_ref, h2_ref, h3_ref, total_ref, part_ref = refs
    else:
        part_ref, dd_ref, h1_ref, h2_ref, h3_ref = refs
    halo = [None, h1_ref, h2_ref, h3_ref]
    _, probes, columns = own[1].shape
    rows = ROWS
    tiles = columns // LANES
    lane = lax.broadcasted_iota(jnp.int32, (GROUP, LANES), 1)
    first, last = lane == 0, lane == LANES - 1
    nothing = jnp.zeros((GROUP, LANES), jnp.float32)
    above_rows, below_rows = reach(chunk)

    def at(c):
        return pl.ds(c * LANES, LANES)

    spans = []
    for level in range(1, ITERS):
        begin, end = level - above_rows, rows + below_rows - level
        spans.append([r for r in range(begin, end) if owner(level, r, rows) == stage])
    upward = below_rows > above_rows
    corner = [3] if upward else [4]
    quads = [corner, range(corner[0] + 1, rows), range(corner[0])][stage]
    low = min(min(spans[0]), min(quads))
    high = max(max(spans[0]), max(quads))

    inside = None
    for r in range(low, high + 1):
        if r < 0:
            ref, row = far_ref, reach(0)[0] * probes + rows + r
        elif r < rows:
            ref, row = up_ref, up_start(CHUNKS, probes) + r
        else:
            ref, row = far_ref, up_start(CHUNKS, probes) + r - rows
        line = ref[row : row + 1, :]
        dd_ref[r - low] = jnp.broadcast_to(line + (4.0 - SHIFT), (GROUP, columns))
        if not 0 <= r < rows:
            inside = jnp.where(jnp.broadcast_to(line[:, :LANES], (GROUP, LANES)) > 0.0, 1.0, 0.0)

    def where(level, r, base):
        mine = pl.ds(base, GROUP)
        if level:
            if not 0 <= r < rows:
                n = r - rows if r >= rows else r + above_rows - level
                return halo[level], (n, mine)
            by = owner(level, r, rows)
            source = own if by == stage else middle
            return source[level], (r - kept(by, level, rows)[0], mine)
        if r < 0:
            return side_ref, (pl.ds((r + above_rows) * probes + base, GROUP),)
        if r >= rows:
            return side_ref, (pl.ds(up_start(chunk, probes) + (r - rows) * probes + base, GROUP),)
        ref, start = edge_of(r, chunk, probes, edges)
        return ref, (pl.ds(start + base, GROUP),)

    def sideways(v):
        left = [pltpu.roll(t, 1, 1) for t in v]
        right = [pltpu.roll(t, LANES - 1, 1) for t in v]
        out = []
        for c in range(tiles):
            a = jnp.where(first, left[c - 1] if c else nothing, left[c])
            b = jnp.where(last, right[c + 1] if c + 1 < tiles else nothing, right[c])
            out.append(a + b)
        return out

    def group(base):
        def line(level, r):
            ref, index = where(level, r, base)
            return [ref[index + (at(c),)] for c in range(tiles)]

        totals = []
        for level, span in enumerate(spans):
            cross, square = nothing, nothing
            before, here = line(level, span[0] - 1), line(level, span[0])
            for r in span:
                after = line(level, r + 1)
                side = sideways(here)
                ref, index = where(level + 1, r, base)
                for c in range(tiles):
                    value = dd_ref[r - low, :, at(c)] * here[c] - (side[c] + (before[c] + after[c]))
                    if not 0 <= r < rows:
                        value = inside * value
                    ref[index + (at(c),)] = value
                    if 0 <= r < rows:
                        cross = cross + here[c] * value
                        square = square + value * value
                before, here = here, after
            totals += [cross, square]
        quad = nothing
        for r in quads:
            here = line(3, r)
            beyond = line(3, r + 1 if upward else r - 1)
            right = [pltpu.roll(t, LANES - 1, 1) for t in here]
            for c in range(tiles):
                beside = jnp.where(last, right[c + 1] if c + 1 < tiles else nothing, right[c]) + beyond[c]
                quad = quad + here[c] * (dd_ref[r - low, :, at(c)] * here[c] - (beside + beside))
        totals.append(quad)
        for k, total in enumerate(totals):
            mine = pl.ds(k * probes + base, GROUP)
            part_ref[mine, :] = total + before_ref[mine, :] if stage else total

    for base in range(0, probes, GROUP):
        group(base)
    part_ref[7 * probes :, :] = jnp.zeros((probes, LANES), jnp.float32)
    if not final:
        return
    for k in range(8):
        begin = k * CHUNKS * probes
        total_ref[begin : begin + probes, :] = earlier_ref[k * probes : (k + 1) * probes, :]
        total_ref[begin + probes : begin + 2 * probes, :] = part_ref[k * probes : (k + 1) * probes, :]
    ones = jnp.ones((GROUP, LANES), jnp.float32)
    line = lax.dot_general(
        ones, total_ref[...], (((1,), (1,)), ((), ())),
        precision=lax.Precision.HIGHEST, preferred_element_type=jnp.float32,
    )
    sums_ref[...] = jnp.broadcast_to(line[None, 0:1, :], sums_ref.shape)


def quadratic(c, moments):
    total = None
    n = len(c)
    for s in range(2 * n - 1):
        pairs = [c[a] * c[s - a] for a in range(max(0, s - n + 1), min(n, s + 1))]
        term = functools.reduce(lambda a, b: a + b, pairs) * moments[s]
        total = term if total is None else total + term
    return total


def coefficients(mu, shift):
    zero = jnp.zeros_like(mu[0])
    size = [jnp.abs(m) for m in mu]
    moved = [mu[k + 1] + shift * mu[k] for k in range(2 * ITERS - 1)]
    moved_size = [size[k + 1] + shift * size[k] for k in range(2 * ITERS - 1)]
    residual = [jnp.ones_like(mu[0])]
    direction = residual
    solution = [zero] * ITERS
    norm_now = mu[0]
    lost = jnp.ones_like(mu[0])
    amplified = zero
    for i in range(ITERS):
        curvature = quadratic(direction, moved)
        step = norm_now / curvature
        loss = quadratic([jnp.abs(d) for d in direction], moved_size) / jnp.abs(curvature)
        length = jnp.sqrt(jnp.abs(quadratic(direction, mu)))
        amplified = amplified + (loss + lost) * (jnp.abs(step) * length)
        solution = [x + step * direction[k] if k <= i else x for k, x in enumerate(solution)]
        if i + 1 < ITERS:
            applied = [shift * d for d in direction] + [zero]
            applied = [a + (direction[k - 1] if k else zero) for k, a in enumerate(applied)]
            residual = [r - step * a for r, a in zip(residual + [zero], applied)]
            norm_next = quadratic(residual, mu)
            lost = quadratic([jnp.abs(r) for r in residual], size) / jnp.abs(norm_next)
            ratio = norm_next / norm_now
            direction = [r + ratio * d for r, d in zip(residual, direction + [zero])]
            norm_now = norm_next
    for k in range(ITERS):
        amplified = amplified + jnp.abs(solution[k]) * jnp.sqrt(size[2 * k])
    length = jnp.sqrt(quadratic(solution, mu))
    return solution, amplified / length


def solve_kernel(cells, groups, sums_ref, coef_ref, trace_ref):
    row = jnp.sum(sums_ref[...], axis=0)
    width = row.shape[1]
    probes = width // 8
    row = jnp.broadcast_to(row, (8, width))
    mu = [jnp.full((8, LANES), cells, jnp.float32)]
    for k in range(2 * ITERS - 1):
        moved = pltpu.roll(row, width - k * probes, 1) if k else row
        mu.append(moved[:, :LANES])
    coef, amplified = coefficients(mu, SHIFT)
    sub = lax.broadcasted_iota(jnp.int32, (8, LANES), 0)
    lane = lax.broadcasted_iota(jnp.int32, (8, LANES), 1)
    packed = jnp.zeros((8, LANES), jnp.float32)
    trace = jnp.zeros((8, LANES), jnp.float32)
    for k in range(ITERS):
        packed = jnp.where(sub == k, coef[k], packed)
        trace = trace + coef[k] * mu[k]
    trace = jnp.where(lane < probes, trace, 0.0)
    total = jnp.sum(trace, axis=1, keepdims=True) / (float(probes * groups) * cells)
    unsafe = jnp.where(amplified < AMPLIFIED, 0.0, 1.0)
    unsafe = jnp.max(jnp.where(lane < probes, unsafe, 0.0), axis=1, keepdims=True)
    both = jnp.where(lane < LANES // 2, jnp.broadcast_to(total, lane.shape), jnp.broadcast_to(unsafe, lane.shape))
    trace_ref[...] = jnp.where(lane < LANES - 1, both, 0.0)[0:1]
    across = jnp.transpose(packed)
    for k in range(ITERS):
        coef_ref[k * probes : (k + 1) * probes, :] = jnp.broadcast_to(across[:probes, k : k + 1], (probes, LANES))


def combine_kernel(coef_ref, *refs):
    edges = refs[: CHUNKS + 2]
    powers = [refs[CHUNKS + 2 + 9 * n : CHUNKS + 11 + 9 * n] for n in range(CHUNKS)]
    out_ref, made_ref, sems = refs[10 * CHUNKS + 2 :]
    probes, rows, columns = made_ref.shape
    count = probes // CHUNKS

    def copy(g):
        mine = pl.ds(g * GROUP, GROUP)
        return pltpu.make_async_copy(made_ref.at[mine], out_ref.at[mine], sems.at[g])

    for g in range(probes // GROUP):
        base = g * GROUP
        chunk, local = divmod(base, count)

        def power(level, r):
            by = owner(level, r, rows)
            return powers[chunk][3 * by + level - 1][r - kept(by, level, rows)[0], mine, at]

        mine = slice(local, local + GROUP)
        c = [coef_ref[k * probes + base : k * probes + base + GROUP, :] for k in range(ITERS)]
        for t in range(columns // LANES):
            at = slice(t * LANES, (t + 1) * LANES)
            made = []
            for r in range(rows):
                ref, start = edge_of(r, chunk, count, edges)
                probe = ref[start + local : start + local + GROUP, at]
                made.append(
                    (c[0] * probe + c[1] * power(1, r)) + (c[2] * power(2, r) + c[3] * power(3, r))
                )
            made_ref[base : base + GROUP, :, at] = jnp.swapaxes(jnp.stack(made), 0, 1)
        copy(g).start()
    for g in range(probes // GROUP):
        copy(g).wait()


def on_device(probe_signs, sensor_mask, sensor_weight, prior_mass):
    probes, rows, columns = probe_signs.shape
    strips = lax.axis_size("space")
    groups = lax.axis_size("probe")
    count = probes // CHUNKS
    params = pltpu.CompilerParams(vmem_limit_bytes=VMEM_LIMIT)

    def shaped(*shape):
        return jax.ShapeDtypeStruct(shape, jnp.float32)

    edges = pl.pallas_call(
        prepare_kernel,
        in_specs=[HBM] * 4,
        out_specs=[VMEM] * (CHUNKS + 2),
        out_shape=[shaped(up_start(CHUNKS, count) + rows, columns), shaped(probes, columns)]
        + [shaped(reach(n)[0] * count + (0 if n else rows), columns) for n in range(CHUNKS)],
        scratch_shapes=[
            pltpu.VMEM((probes, rows, columns), jnp.int32),
            pltpu.VMEM((rows, columns), jnp.int32),
            pltpu.VMEM((rows, columns), jnp.float32),
            pltpu.VMEM((rows, columns), jnp.float32),
            pltpu.SemaphoreType.DMA((probes // GROUP + 3,)),
        ],
        compiler_params=params,
    )(probe_signs, sensor_mask, sensor_weight, prior_mass)
    up, mid, *downs = edges
    below = lax.ppermute(up, "space", [(i + 1, i) for i in range(strips - 1)])
    above = []
    for dn in downs:
        above.append(lax.ppermute(dn, "space", [(i, i + 1) for i in range(strips - 1)]))

    made = [[], []]
    parts = [None, None]
    for stage in range(3):
        for n in range(CHUNKS):
            final = stage == 2 and n == CHUNKS - 1
            args = [up, mid, downs[n]]
            if stage:
                args += [below, below] if stage == 1 else [above[n], above[0]]
                args += [*made[n][:3], parts[n]]
            if final:
                args.append(parts[0])
            outs = [shaped(kept(stage, level, rows)[1], count, columns) for level in range(1, ITERS)]
            outs.append(shaped(strips, 1, 8 * probes) if final else shaped(8 * count, LANES))
            scratch = [pltpu.VMEM((rows + 5, GROUP, columns), jnp.float32)]
            scratch += [pltpu.VMEM((size, count, columns), jnp.float32) for size in (3, 2, 1)]
            if final:
                scratch += [pltpu.VMEM((8 * probes, LANES), jnp.float32), pltpu.VMEM((8 * count, LANES), jnp.float32)]
            *fresh, parts[n] = pl.pallas_call(
                functools.partial(powers_kernel, stage, n, final),
                in_specs=[VMEM] * len(args),
                out_specs=[VMEM] * len(outs),
                out_shape=outs,
                scratch_shapes=scratch,
                compiler_params=params,
            )(*args)
            made[n] += fresh

    sums = lax.all_to_all(parts[-1], "space", split_axis=0, concat_axis=0, tiled=True)

    cells = float(rows * strips * columns)
    coef, trace = pl.pallas_call(
        functools.partial(solve_kernel, cells, groups),
        in_specs=[VMEM],
        out_specs=[VMEM, VMEM],
        out_shape=[shaped(ITERS * probes, LANES), shaped(1, LANES)],
        compiler_params=params,
    )(sums)

    one, two, three = [
        lax.ppermute(trace, "probe", [(i, (i + k) % groups) for i in range(groups)])
        for k in range(1, groups)
    ]

    args = [coef, *edges]
    for fresh in made:
        args += fresh
    combined = pl.pallas_call(
        combine_kernel,
        in_specs=[VMEM] * len(args),
        out_specs=HBM,
        out_shape=shaped(probes, rows, columns),
        scratch_shapes=[
            pltpu.VMEM((probes, rows, columns), jnp.float32),
            pltpu.SemaphoreType.DMA((probes // GROUP,)),
        ],
        compiler_params=params,
        cost_estimate=pl.CostEstimate(
            flops=8 * probes * rows * columns, bytes_accessed=20 * probes * rows * columns, transcendentals=0
        ),
    )(*args)

    everyone = (trace + two) + (one + three)

    def again(state):
        _, turn, _, _ = state
        past = turn.astype(jnp.int32)
        diagonal = (sensor_mask + past).astype(jnp.float32) * sensor_weight + prior_mass
        made, cell = iterate_on_device(probe_signs + past, diagonal)
        return turn, turn + 1.0, made, cell

    state = (everyone[0, LANES // 2], everyone[0, LANES - 1], combined, everyone[0, 0])
    return lax.while_loop(lambda state: state[0] > 0.0, again, state)[2:]


def solution(mesh):
    return jax.shard_map(
        on_device,
        mesh=mesh,
        in_specs=(P("probe", "space", None), P("space", None), P("space", None), P("space", None)),
        out_specs=(P("probe", "space", None), P()),
        check_vma=False,
    )
```
